1024 devices in a mesh: ctx: 128 (over z_lo, x, core), tp: 8 (over y, z_hi).
Axes of the slice: x: 4, y: 4, z: 32 (z_hi: 2, z_lo: 16; z = z_hi * 16 + z_lo), core: 2. Of those that a mesh axis runs over, the one named last changes fastest.
Arguments:
- hidden_in: bfloat16 [32768, 4096], P(('ctx', 'tp')), may hold values from -6 to 6
- norm_gain: float32 [4096], replicated, may hold values from 0.5 to 1.5
- proj_weight: bfloat16 [4096, 8192], P(None, 'tp'), may hold values from -0.0625 to 0.0625
- conv_in: bfloat16 [32768, 8192], P('ctx', 'tp'), may hold values from -6 to 6
- conv_weight: float32 [4, 8192], P(None, 'tp'), may hold values from -3 to 3
- conv_bias: float32 [8192], P('tp'), may hold values from -3 to 3
- act_grad: bfloat16 [32768, 8192], P('ctx', 'tp'), may hold values from -6 to 6
Outputs:
- hidden_input_gradient: bfloat16 [32768, 4096], P(('ctx', 'tp'))
- norm_gain_gradient: float32 [4096], replicated
- taps_grad: float32 [4, 8192], P(None, 'tp')
- bias_grad: float32 [8192], P('tp')
The draws below stay inside these ranges and needn't reach their ends.
All inputs are finite; a program needn't handle non-finite values.
Results may differ from the reference program's by a relative error of at most 0.013.
Values may be sent and summed in bfloat16 or wider, within the bound.
A program may use at most 32 MiB of HBM per device.

```python
import jax
import jax.numpy as jnp
from jax import lax

D = 4096
INNER_DEV = 1024
TAPS = 4
TOKENS = 32768
INNER = 8192
N_TP = 8


def block_levels(key, extent, pieces, low, largest):
    def one(dim, blocks):
        steps = jax.random.uniform(jax.random.fold_in(jax.random.fold_in(key, 6), dim), (blocks,), jnp.float32, low / len(pieces), largest / len(pieces))
        return jnp.repeat(jnp.exp(steps), extent[dim] // blocks).reshape((-1,) + (1,) * (len(extent) - dim - 1))

    loudness = one(*pieces[0])
    for cut in pieces[1:]:
        loudness = loudness * one(*cut)
    return loudness


def gaussian(key, dims, scale, reach, split=(), kind=jnp.bfloat16):
    factor_of = block_levels(key, dims, split, -0.22, 0.18) if split else 1.0
    values = jax.random.normal(key, dims, jnp.float32) * scale * factor_of
    return jnp.minimum(jnp.maximum(values, -reach), reach).astype(kind)


def setup_inputs(seed: int = 0) -> dict:
    seeds = jax.random.split(jax.random.key(seed), 8)
    hidden_in = gaussian(seeds[0], (TOKENS, D), 1.0, 6.0, ((0, 1024),))
    norm_gain = jnp.clip(1.0 + 0.1 * jax.random.normal(seeds[1], (D,), jnp.float32), 0.5, 1.5)
    proj_weight = gaussian(seeds[2], (D, INNER), INNER ** -0.5, 0.0625, ((1, 8),))
    conv_in = gaussian(seeds[3], (TOKENS, INNER), 1.0, 6.0, ((0, 128), (1, 8)))
    conv_weight = gaussian(seeds[4], (TAPS, INNER), 0.5, 3.0, ((1, 8),), jnp.float32)
    conv_bias = gaussian(seeds[5], (INNER,), 0.5, 3.0, ((0, 8),), jnp.float32)
    act_grad = gaussian(seeds[6], (TOKENS, INNER), 1.0, 6.0, ((0, 128), (1, 8)))
    return {"hidden_in": hidden_in, "norm_gain": norm_gain, "proj_weight": proj_weight, "conv_in": conv_in, "conv_weight": conv_weight, "conv_bias": conv_bias, "act_grad": act_grad}


def channel_block(carry, items):
    saved, cotangent, taps, offset, weight = items
    count_tok = saved.shape[0]
    tap_count = taps.shape[0]
    padded = jnp.concatenate([jnp.zeros((tap_count - 1, saved.shape[1]), jnp.float32), saved.astype(jnp.float32)], 0)
    preact = offset[None, :] + sum((taps[index][None, :] * padded[tap_count - 1 - index:tap_count - 1 - index + count_tok] for index in range(tap_count)))
    sigmoid_v = jax.nn.sigmoid(preact)
    pre_grad = cotangent.astype(jnp.float32) * sigmoid_v * (1.0 + preact * (1.0 - sigmoid_v))
    taps_part = jnp.stack([lax.optimization_barrier(jnp.sum(pre_grad * padded[tap_count - 1 - index:tap_count - 1 - index + count_tok], 0)) for index in range(tap_count)], 0)
    bias_part = lax.optimization_barrier(jnp.sum(pre_grad, 0))
    after = jnp.concatenate([pre_grad, jnp.zeros((tap_count - 1, saved.shape[1]), jnp.float32)], 0)
    in_grad = sum((taps[index][None, :] * after[index:index + count_tok] for index in range(tap_count))).astype(jnp.bfloat16)
    part_grad = lax.dot_general(in_grad, weight, (((1,), (1,)), ((), ())), preferred_element_type=jnp.float32).astype(jnp.bfloat16)
    part_grad = lax.optimization_barrier(part_grad)
    carry = carry + part_grad.astype(jnp.float32)
    return (carry, (taps_part, bias_part))

def reference(hidden_in, norm_gain, proj_weight, conv_in, conv_weight, conv_bias, act_grad):
    count_tok = conv_in.shape[0]
    blocks = N_TP
    width = INNER_DEV
    saved = conv_in.reshape(count_tok, blocks, width).transpose(1, 0, 2)
    cotangent = act_grad.reshape(count_tok, blocks, width).transpose(1, 0, 2)
    taps = conv_weight.reshape(TAPS, blocks, width).transpose(1, 0, 2)
    offset = conv_bias.reshape(blocks, width)
    weight = proj_weight.reshape(D, blocks, width).transpose(1, 0, 2)
    start_sum = jnp.zeros((count_tok, D), jnp.float32)
    normalized_gradient, parts = lax.scan(channel_block, start_sum, (saved, cotangent, taps, offset, weight))
    taps_grad = parts[0].transpose(1, 0, 2).reshape(TAPS, blocks * width)
    bias_grad = parts[1].reshape(blocks * width)
    hidden_state = hidden_in.astype(jnp.float32)
    root_mean_square = jnp.sqrt(lax.optimization_barrier(jnp.mean(hidden_state * hidden_state, -1, keepdims=True)) + 1e-05)
    normalized_input = hidden_state / root_mean_square
    norm_gain_gradient = lax.optimization_barrier(jnp.sum(normalized_gradient * normalized_input, 0))
    scaled_gradient = norm_gain[None, :] * normalized_gradient
    mean_correction = lax.optimization_barrier(jnp.mean(scaled_gradient * normalized_input, -1, keepdims=True))
    hidden_input_gradient = ((scaled_gradient - normalized_input * mean_correction) / root_mean_square).astype(jnp.bfloat16)
    return (hidden_input_gradient, norm_gain_gradient, taps_grad, bias_grad)
```

```python
import jax
import jax.numpy as jnp
from jax import lax
from jax.experimental import pallas as pl
from jax.experimental.pallas import tpu as pltpu
from jax.sharding import Mesh
from jax.sharding import PartitionSpec as P

MESH = pl.DeviceIdType.MESH
NZL, NX, NC, NY, NZH = 16, 4, 2, 4, 2
NZ = NZL * NZH
NPLANE = NX * NC * NY
NLINE = NX * NC
NCTX = NZL * NX * NC
ROWS = 256
CHAN = 1024
DIM = 4096
NCH = 8
WIDE = DIM // NCH
PER = WIDE // 128
OWN = 32
PAIR = 64
TILE = 16
NEAR = 4
F32 = jnp.float32
BF16 = jnp.bfloat16


def rem(a, b):
    return lax.rem(a, b)


def z_device(z):
    z = rem(z, NZ)
    return {"zh": z // NZL, "zl": rem(z, NZL)}


def plane_device(q):
    return {"x": q // (NY * NC), "y": rem(q // NC, NY), "c": rem(q, NC)}


def line_device(q):
    return {"x": q // NC, "c": rem(q, NC)}


def ctx_device(n):
    return {"zl": n // NLINE, "x": rem(n // NC, NX), "c": rem(n, NC)}


def kernel(
    hid_h, gain_h, w_h, conv_h, cw_h, cb_h, act_h,
    out_h, gain_o, taps_o, bias_o,
    hid, gain, w, conv, cw, cb, act, out,
    hprev, hconv, hact,
    xf, pg, ing, tacc,
    pbuf, ybuf, own, zs, zr, inv,
    gbuf, gr, za, ga, tpc, tr, tz, tf,
    in_sem, w_sem, out_sem, hs_sem, hr_sem, ys_sem, yr_sem, zs_sem, zr_sem, small_s, small_r, far,
):
    zl = lax.axis_index("zl")
    zh = lax.axis_index("zh")
    x = lax.axis_index("x")
    y = lax.axis_index("y")
    c = lax.axis_index("c")
    z = zh * NZL + zl
    q = (x * NY + y) * NC + c
    line = x * NC + c
    n = zl * NLINE + line
    has_next = n < NCTX - 1
    has_prev = n > 0
    far_next = jnp.logical_and(line == NLINE - 1, has_next)
    far_prev = jnp.logical_and(line == 0, has_prev)

    def remote(src, dst, send, recv, device):
        return pltpu.make_async_remote_copy(
            src_ref=src, dst_ref=dst, send_sem=send, recv_sem=recv, device_id=device, device_id_type=MESH
        )

    def drain(ref, sem):
        pltpu.make_async_copy(ref, ref, sem).wait()

    loads = [
        pltpu.make_async_copy(a, b, in_sem.at[i])
        for i, (a, b) in enumerate(
            [(conv_h, conv), (act_h, act), (cw_h, cw), (cb_h, cb), (hid_h, hid), (gain_h, gain)]
        )
    ]
    for load in loads:
        load.start()

    def w_load(j):
        rows = pl.ds(pl.multiple_of(j * WIDE, WIDE), WIDE)
        return pltpu.make_async_copy(w_h.at[rows], w.at[rows], w_sem.at[j])

    @pl.loop(0, NCH)
    def _(j):
        w_load(j).start()

    barrier = pltpu.get_barrier_semaphore()

    @pl.when(has_next)
    def _():
        @pl.when(far_next)
        def _():
            pl.semaphore_signal(barrier, 1, device_id=ctx_device(n + 1), device_id_type=MESH)

    @pl.when(far_prev)
    def _():
        pl.semaphore_signal(barrier, 1, device_id=ctx_device(n - 1), device_id_type=MESH)

    @pl.loop(1, NPLANE)
    def _(k):
        pl.semaphore_signal(barrier, 1, device_id=plane_device(rem(q + k, NPLANE)), device_id_type=MESH)

    @pl.loop(1, NEAR + 1)
    def _(k):
        pl.semaphore_signal(barrier, 1, device_id=z_device(z + k), device_id_type=MESH)
        pl.semaphore_signal(barrier, 1, device_id=z_device(z + NZ - k), device_id_type=MESH)

    xf[0:8, :] = jnp.zeros((8, CHAN), F32)
    tacc[...] = jnp.zeros_like(tacc)
    loads[0].wait()

    @pl.loop(0, ROWS // TILE)
    def _(i):
        t = pl.multiple_of(i * TILE, TILE)
        xf[pl.ds(t + 8, TILE), :] = conv[pl.ds(t, TILE), :].astype(F32)

    for load in loads[1:4]:
        load.wait()

    def grad_tile(t, rows, cotangent):
        above = xf[pl.ds(t, rows + 8), :]
        xs = [above[8 - k : 8 - k + rows] for k in range(4)]
        pre = cb[0:1, :] + sum(cw[k : k + 1, :] * xs[k] for k in range(4))
        s = 1.0 / (1.0 + jnp.exp(-pre))
        return cotangent * s * (1.0 + pre * (1.0 - s)), xs

    def pass_one(i):
        t = pl.multiple_of(i * TILE, TILE)
        g, xs = grad_tile(t, TILE, act[pl.ds(t, TILE), :].astype(F32))
        pg[pl.ds(t, TILE), :] = g
        for k in range(5):
            term = g * xs[k] if k < 4 else g
            tacc[k] += term[0:8] + term[8:16]

    def pass_two(i):
        t = pl.multiple_of(i * TILE, TILE)
        below = pg[pl.ds(t, TILE + 8), :]
        total = sum(cw[k : k + 1, :] * below[k : k + TILE] for k in range(4))
        ing[pl.ds(t, TILE), :] = total.astype(BF16)

    last = ROWS // TILE - 1

    @pl.loop(1, last // 2)
    def _(i):
        pass_one(i)

    pl.semaphore_wait(
        barrier,
        NPLANE - 1 + 2 * NEAR + jnp.where(far_next, 1, 0) + jnp.where(far_prev, 1, 0),
    )
    to_next = remote(conv.at[pl.ds(ROWS - 16, 16)], hprev, hs_sem.at[0], hr_sem.at[0], ctx_device(jnp.minimum(n + 1, NCTX - 1)))
    to_prev = [
        remote(conv.at[pl.ds(0, 16)], hconv, hs_sem.at[1], hr_sem.at[1], ctx_device(jnp.maximum(n - 1, 0))),
        remote(act.at[pl.ds(0, 16)], hact, hs_sem.at[2], hr_sem.at[2], ctx_device(jnp.maximum(n - 1, 0))),
    ]

    @pl.when(has_next)
    def _():
        to_next.start()

    @pl.when(has_prev)
    def _():
        for copy in to_prev:
            copy.start()

    for step in (NEAR, NZ - NEAR):
        pl.semaphore_signal(far.at[0], 1, device_id=z_device(z + step), device_id_type=MESH)

    @pl.loop(last // 2, last + 1)
    def _(i):
        pass_one(i)

    @pl.loop(1, last)
    def _(i):
        pass_two(i)

    pl.semaphore_wait(far.at[0], 2)
    for step in (2 * NEAR, NZ - 2 * NEAR):
        pl.semaphore_signal(far.at[1], 1, device_id=z_device(z + step), device_id_type=MESH)

    @pl.when(has_prev)
    def _():
        to_next.wait_recv()
        xf[0:8, :] = hprev[8:16, :].astype(F32)

    pass_one(0)
    pass_two(0)

    @pl.when(has_next)
    def _():
        for copy in to_prev:
            copy.wait_recv()
        xf[ROWS + 8 : ROWS + 16, :] = hconv[0:8, :].astype(F32)
        g, _ = grad_tile(ROWS, 8, hact[0:8, :].astype(F32))
        pg[ROWS : ROWS + 8, :] = g

    @pl.when(jnp.logical_not(has_next))
    def _():
        pg[ROWS : ROWS + 8, :] = jnp.zeros((8, CHAN), F32)

    pass_two(last)

    def product(j):
        rows = pl.ds(pl.multiple_of(j * WIDE, WIDE), WIDE)
        w_load(j).wait()
        part = lax.dot_general(ing[...], w[rows, :], (((1,), (1,)), ((), ())), preferred_element_type=F32)
        pbuf[j] = part.astype(BF16)

    def y_copy(j, k):
        to = rem(y + k, NY)
        return remote(
            pbuf.at[j, pl.ds(pl.multiple_of(to * PAIR, PAIR), PAIR)],
            ybuf.at[j, y],
            ys_sem.at[j],
            yr_sem.at[j],
            {"y": to},
        )

    def y_send(j):
        for k in range(1, NY):
            y_copy(j, k).start()

    product(0)

    @pl.loop(1, NCH)
    def _(j):
        product(j)
        y_send(j - 1)

    y_send(NCH - 1)

    sums = [jnp.sum(tacc[k], 0, keepdims=True) for k in range(5)]
    for p in range(NLINE):
        for k in range(5):
            tpc[p, k : k + 1, :] = sums[k][:, p * 128 : (p + 1) * 128]
        tpc[p, 5:8, :] = jnp.zeros((3, 128), F32)
    tr[line] = tpc[line]

    loads[4].wait()
    loads[5].wait()

    def squares(j, total):
        cols = pl.ds(pl.multiple_of(j * WIDE, WIDE), WIDE)
        h = hid[:, cols].astype(F32)
        h = h * h
        return total + sum(h[:, i * 128 : (i + 1) * 128] for i in range(PER))

    square = lax.fori_loop(0, NCH, squares, jnp.zeros((OWN, 128), F32))
    rms = jnp.sqrt(jnp.sum(square, -1, keepdims=True) * (1.0 / DIM) + 1e-05)
    inv[...] = jnp.broadcast_to(1.0 / rms, (OWN, 128))

    def line_copy(k, src, dst, i):
        return remote(src, dst, small_s.at[i], small_r.at[i], line_device(rem(line + k, NLINE)))

    @pl.loop(1, NLINE)
    def _(k):
        line_copy(k, tpc.at[rem(line + k, NLINE)], tr.at[line], 0).start()

    pl.semaphore_wait(far.at[1], 2)

    def z_copy(j):
        return remote(zs.at[j], zr.at[j], zs_sem.at[j], zr_sem.at[j], {"zh": 1 - zh})

    mine = pl.multiple_of(zh * OWN, OWN)
    other = pl.multiple_of((1 - zh) * OWN, OWN)

    @pl.loop(0, NCH)
    def _(j):
        drain(ybuf.at[j, pl.ds(0, NY - 1)], yr_sem.at[j])
        ybuf[j, y] = pbuf[j, pl.ds(pl.multiple_of(y * PAIR, PAIR), PAIR), :]

        def total(start):
            return sum(ybuf[j, s, pl.ds(start, OWN), :].astype(F32) for s in range(NY))

        zs[j] = total(other).astype(BF16)
        own[j] = total(mine)
        z_copy(j).start()

    drain(tr.at[pl.ds(0, NLINE - 1)], small_r.at[0])
    tz[zl] = jnp.sum(tr[...], 0)

    def zl_copy(k):
        to = rem(zl + k, NZL)
        return remote(tz.at[zl], tz.at[zl], small_s.at[1], small_r.at[1], {"zl": to})

    @pl.loop(1, NZL)
    def _(k):
        zl_copy(k).start()

    def xhat_of(j):
        cols = pl.ds(pl.multiple_of(j * WIDE, WIDE), WIDE)
        return hid[:, cols].astype(F32) * inv[:, 0:1]

    def gain_of(j):
        return gain[0:1, pl.ds(pl.multiple_of(j * WIDE, WIDE), WIDE)]

    def arrive(j, mean):
        z_copy(j).wait_recv()
        normed = own[j] + zr[j].astype(F32)
        own[j] = normed
        both = normed * xhat_of(j)
        sums = jnp.sum(both, 0, keepdims=True)
        for i in range(PER):
            gbuf[j * PER + i, 0:1, :] = sums[:, i * 128 : (i + 1) * 128]
        both = both * gain_of(j)
        mean = mean + sum(both[:, i * 128 : (i + 1) * 128] for i in range(PER))

        @pl.loop(0, PER)
        def _(i):
            p = j * PER + i

            @pl.when(p != q)
            def _():
                remote(
                    gbuf.at[p, pl.ds(0, 1)], gr.at[q, pl.ds(0, 1)], small_s.at[2], small_r.at[2], plane_device(p)
                ).start()

            @pl.when(p == q)
            def _():
                gr[q, 0:1, :] = gbuf[p, 0:1, :]

        return mean

    mean = lax.fori_loop(0, NCH, arrive, jnp.zeros((OWN, 128), F32))
    mean = jnp.sum(mean, -1, keepdims=True) * (1.0 / DIM)

    drain(tz.at[pl.ds(0, NZL - 1)], small_r.at[1])
    tf[line] = jnp.sum(tz[...], 0)

    drain(gr.at[pl.ds(0, NPLANE - 1), pl.ds(0, 1)], small_r.at[2])
    za[z, 0:1, :] = jnp.sum(gr[:, 0:1, :], 0)

    @pl.loop(1, NLINE)
    def _(k):
        line_copy(k, tf.at[line], tf.at[line], 3).start()

    @pl.loop(1, NZ)
    def _(k):
        remote(
            za.at[z, pl.ds(0, 1)], za.at[z, pl.ds(0, 1)], small_s.at[4], small_r.at[4], z_device(z + k)
        ).start()

    @pl.loop(0, NCH)
    def _(j):
        cols = pl.ds(pl.multiple_of(j * WIDE, WIDE), WIDE)
        value = (gain_of(j) * own[j] - xhat_of(j) * mean) * inv[:, 0:1]
        out[:, cols] = value.astype(BF16)

    store = pltpu.make_async_copy(out, out_h, out_sem)
    store.start()

    drain(tf.at[pl.ds(0, NLINE - 1)], small_r.at[3])
    for p in range(NLINE):
        taps_o[:, p * 128 : (p + 1) * 128] = tf[p, 0:4, :]
        bias_o[:, p * 128 : (p + 1) * 128] = tf[p, 4:5, :]

    drain(za.at[pl.ds(0, NZ - 1), pl.ds(0, 1)], small_r.at[4])
    ga[q, 0:1, :] = jnp.sum(za[:, 0:1, :], 0)

    @pl.loop(1, NPLANE)
    def _(k):
        remote(
            ga.at[q, pl.ds(0, 1)], ga.at[q, pl.ds(0, 1)], small_s.at[5], small_r.at[5], plane_device(rem(q + k, NPLANE))
        ).start()

    @pl.when(has_next)
    def _():
        to_next.wait_send()

    @pl.when(has_prev)
    def _():
        for copy in to_prev:
            copy.wait_send()

    @pl.loop(0, NCH)
    def _(j):
        drain(ybuf.at[j, pl.ds(0, NY - 1)], ys_sem.at[j])
        z_copy(j).wait_send()

    drain(tr.at[pl.ds(0, NLINE - 1)], small_s.at[0])
    drain(tz.at[pl.ds(0, NZL - 1)], small_s.at[1])
    drain(gr.at[pl.ds(0, NPLANE - 1), pl.ds(0, 1)], small_s.at[2])
    drain(tf.at[pl.ds(0, NLINE - 1)], small_s.at[3])
    drain(za.at[pl.ds(0, NZ - 1), pl.ds(0, 1)], small_s.at[4])
    store.wait()
    drain(ga.at[pl.ds(0, NPLANE - 1), pl.ds(0, 1)], small_r.at[5])
    gain_o[...] = ga[:, 0, :]
    drain(ga.at[pl.ds(0, NPLANE - 1), pl.ds(0, 1)], small_s.at[5])


def on_device(hidden_in, norm_gain, proj_weight, conv_in, conv_weight, conv_bias, act_grad):
    vmem = pltpu.VMEM
    dma = pltpu.SemaphoreType.DMA
    out, gain, taps, bias = pl.pallas_call(
        kernel,
        out_shape=(
            jax.ShapeDtypeStruct((OWN, DIM), BF16),
            jax.ShapeDtypeStruct((NPLANE, 128), F32),
            jax.ShapeDtypeStruct((4, CHAN), F32),
            jax.ShapeDtypeStruct((1, CHAN), F32),
        ),
        in_specs=[pl.BlockSpec(memory_space=pl.ANY)] * 7,
        out_specs=(pl.BlockSpec(memory_space=pl.ANY),) + (pl.BlockSpec(memory_space=vmem),) * 3,
        scratch_shapes=[
            vmem((OWN, DIM), BF16),
            vmem((1, DIM), F32),
            vmem((DIM, CHAN), BF16),
            vmem((ROWS, CHAN), BF16),
            vmem((4, CHAN), F32),
            vmem((1, CHAN), F32),
            vmem((ROWS, CHAN), BF16),
            vmem((OWN, DIM), BF16),
            vmem((16, CHAN), BF16),
            vmem((16, CHAN), BF16),
            vmem((16, CHAN), BF16),
            vmem((ROWS + 16, CHAN), F32),
            vmem((ROWS + 8, CHAN), F32),
            vmem((ROWS, CHAN), BF16),
            vmem((5, 8, CHAN), F32),
            vmem((NCH, ROWS, WIDE), BF16),
            vmem((NCH, NY, PAIR, WIDE), BF16),
            vmem((NCH, OWN, WIDE), F32),
            vmem((NCH, OWN, WIDE), BF16),
            vmem((NCH, OWN, WIDE), BF16),
            vmem((OWN, 128), F32),
            vmem((NPLANE, 8, 128), F32),
            vmem((NPLANE, 8, 128), F32),
            vmem((NZ, 8, 128), F32),
            vmem((NPLANE, 8, 128), F32),
            vmem((NLINE, 8, 128), F32),
            vmem((NLINE, 8, 128), F32),
            vmem((NZL, 8, 128), F32),
            vmem((NLINE, 8, 128), F32),
            dma((6,)),
            dma((NCH,)),
            dma,
            dma((3,)),
            dma((3,)),
            dma((NCH,)),
            dma((NCH,)),
            dma((NCH,)),
            dma((NCH,)),
            dma((6,)),
            dma((6,)),
            pltpu.SemaphoreType.REGULAR((2,)),
        ],
        compiler_params=pltpu.CompilerParams(collective_id=0, has_side_effects=True),
        name="layer_backward",
    )(
        hidden_in,
        norm_gain.reshape(1, DIM),
        proj_weight,
        conv_in,
        conv_weight,
        conv_bias.reshape(1, CHAN),
        act_grad,
    )
    return out, gain.reshape(DIM), taps, bias.reshape(CHAN)


def solution(mesh):
    finer = Mesh(mesh.devices.reshape(NZL, NX, NC, NY, NZH), ("zl", "x", "c", "y", "zh"))
    ctx = ("zl", "x", "c")
    tp = ("y", "zh")
    return jax.shard_map(
        on_device,
        mesh=finer,
        in_specs=(
            P(ctx + tp, None),
            P(),
            P(None, tp),
            P(ctx, tp),
            P(None, tp),
            P(tp),
            P(ctx, tp),
        ),
        out_specs=(P(ctx + tp, None), P(), P(None, tp), P(tp)),
        check_vma=False,
    )
```

```python
import jax
import jax.numpy as jnp
from jax import lax
from jax.experimental import pallas as pl
from jax.experimental.pallas import tpu as pltpu
from jax.sharding import Mesh
from jax.sharding import PartitionSpec as P

MESH = pl.DeviceIdType.MESH
NZL, NX, NC, NY, NZH = 16, 4, 2, 4, 2
NZ = NZL * NZH
NPLANE = NX * NC * NY
NLINE = NX * NC
NCTX = NZL * NX * NC
ROWS = 256
CHAN = 1024
DIM = 4096
NCH = 16
WIDE = DIM // NCH
PER = WIDE // 128
OWN = 32
PAIR = 64
TILE = 16
NEAR = 4
WINDOW = 8
FIRST = 10
GROUP = 4
F32 = jnp.float32
BF16 = jnp.bfloat16


def rem(a, b):
    return lax.rem(a, b)


def z_device(z):
    z = rem(z, NZ)
    return {"zh": z // NZL, "zl": rem(z, NZL)}


def plane_device(q):
    return {"x": q // (NY * NC), "y": rem(q // NC, NY), "c": rem(q, NC)}


def line_device(q):
    return {"x": q // NC, "c": rem(q, NC)}


def ctx_device(n):
    return {"zl": n // NLINE, "x": rem(n // NC, NX), "c": rem(n, NC)}


def kernel(
    hid_h, gain_h, w_h, conv_h, cw_h, cb_h, act_h,
    out_o, gain_o, taps_o, bias_o,
    hid, gain, w, conv, cw, cb, act,
    hprev, hconv, hact,
    xf, pg, ing, tacc,
    pbuf, ybuf, own, zs, zr, inv, mean,
    gbuf, gr, za, ga, tpc, tr, tn, tz, tf,
    in_sem, w_sem, hs_sem, hr_sem, ys_sem, yr_sem, zs_sem, zr_sem, small_s, small_r, far,
):
    zl = lax.axis_index("zl")
    zh = lax.axis_index("zh")
    x = lax.axis_index("x")
    y = lax.axis_index("y")
    c = lax.axis_index("c")
    z = zh * NZL + zl
    q = (x * NY + y) * NC + c
    line = x * NC + c
    n = zl * NLINE + line
    has_next = n < NCTX - 1
    has_prev = n > 0
    far_next = jnp.logical_and(line == NLINE - 1, has_next)
    far_prev = jnp.logical_and(line == 0, has_prev)

    def remote(src, dst, send, recv, device):
        return pltpu.make_async_remote_copy(
            src_ref=src, dst_ref=dst, send_sem=send, recv_sem=recv, device_id=device, device_id_type=MESH
        )

    def drain(ref, sem):
        pltpu.make_async_copy(ref, ref, sem).wait()

    loads = [
        pltpu.make_async_copy(a, b, in_sem.at[i])
        for i, (a, b) in enumerate(
            [(conv_h, conv), (act_h, act), (cw_h, cw), (cb_h, cb), (hid_h, hid), (gain_h, gain)]
        )
    ]
    for load in loads[:4]:
        load.start()

    barrier = pltpu.get_barrier_semaphore()

    @pl.loop(0, NEAR)
    def _(k):
        pl.semaphore_signal(barrier, 1, device_id=z_device(z + (NEAR - k)), device_id_type=MESH)
        pl.semaphore_signal(barrier, 1, device_id=z_device(z + NZ - (NEAR - k)), device_id_type=MESH)

    @pl.loop(1, NPLANE)
    def _(k):
        pl.semaphore_signal(barrier, 1, device_id=plane_device(rem(q + k, NPLANE)), device_id_type=MESH)

    @pl.when(has_next)
    def _():
        @pl.when(far_next)
        def _():
            pl.semaphore_signal(barrier, 1, device_id=ctx_device(n + 1), device_id_type=MESH)

    @pl.when(far_prev)
    def _():
        pl.semaphore_signal(barrier, 1, device_id=ctx_device(n - 1), device_id_type=MESH)


    for load in loads[4:]:
        load.start()

    def w_load(j):
        rows = pl.ds(pl.multiple_of(j * WIDE, WIDE), WIDE)
        return pltpu.make_async_copy(w_h.at[rows], w.at[rows], w_sem.at[j])

    @pl.loop(0, NCH)
    def _(j):
        w_load(j).start()

    xf[0:8, :] = jnp.zeros((8, CHAN), F32)
    tacc[...] = jnp.zeros_like(tacc)
    loads[0].wait()

    @pl.loop(0, ROWS // TILE)
    def _(i):
        t = pl.multiple_of(i * TILE, TILE)
        xf[pl.ds(t + 8, TILE), :] = conv[pl.ds(t, TILE), :].astype(F32)

    for load in loads[1:4]:
        load.wait()

    def grad_tile(t, rows, cotangent):
        above = xf[pl.ds(t, rows + 8), :]
        xs = [above[8 - k : 8 - k + rows] for k in range(4)]
        pre = cb[0:1, :] + sum(cw[k : k + 1, :] * xs[k] for k in range(4))
        s = 1.0 / (1.0 + jnp.exp(-pre))
        return cotangent * s * (1.0 + pre * (1.0 - s)), xs

    def pass_one(i):
        t = pl.multiple_of(i * TILE, TILE)
        g, xs = grad_tile(t, TILE, act[pl.ds(t, TILE), :].astype(F32))
        pg[pl.ds(t, TILE), :] = g
        for k in range(5):
            term = g * xs[k] if k < 4 else g
            tacc[k] += term[0:8] + term[8:16]

    def pass_two(i):
        t = pl.multiple_of(i * TILE, TILE)
        below = pg[pl.ds(t, TILE + 8), :]
        total = sum(cw[k : k + 1, :] * below[k : k + TILE] for k in range(4))
        ing[pl.ds(t, TILE), :] = total.astype(BF16)

    last = ROWS // TILE - 1

    @pl.loop(1, last + 1)
    def _(i):
        pass_one(i)

    @pl.loop(1, last)
    def _(i):
        pass_two(i)

    pl.semaphore_wait(
        barrier,
        NPLANE - 1 + 2 * NEAR + jnp.where(far_next, 1, 0) + jnp.where(far_prev, 1, 0),
    )
    for step in (NEAR, NZ - NEAR):
        pl.semaphore_signal(far.at[0], 1, device_id=z_device(z + step), device_id_type=MESH)

    to_next = remote(conv.at[pl.ds(ROWS - 16, 16)], hprev, hs_sem.at[0], hr_sem.at[0], ctx_device(jnp.minimum(n + 1, NCTX - 1)))
    to_prev = [
        remote(conv.at[pl.ds(0, 16)], hconv, hs_sem.at[1], hr_sem.at[1], ctx_device(jnp.maximum(n - 1, 0))),
        remote(act.at[pl.ds(0, 16)], hact, hs_sem.at[2], hr_sem.at[2], ctx_device(jnp.maximum(n - 1, 0))),
    ]

    @pl.when(has_next)
    def _():
        to_next.start()

    @pl.when(has_prev)
    def _():
        for copy in to_prev:
            copy.start()

    pl.semaphore_wait(far.at[0], 2)
    for step in (2 * NEAR, NZ - 2 * NEAR):
        pl.semaphore_signal(far.at[1], 1, device_id=z_device(z + step), device_id_type=MESH)

    @pl.when(has_prev)
    def _():
        to_next.wait_recv()
        xf[0:8, :] = hprev[8:16, :].astype(F32)

    pass_one(0)
    pass_two(0)

    @pl.when(has_next)
    def _():
        for copy in to_prev:
            copy.wait_recv()
        xf[ROWS + 8 : ROWS + 16, :] = hconv[0:8, :].astype(F32)
        g, _ = grad_tile(ROWS, 8, hact[0:8, :].astype(F32))
        pg[ROWS : ROWS + 8, :] = g

    @pl.when(jnp.logical_not(has_next))
    def _():
        pg[ROWS : ROWS + 8, :] = jnp.zeros((8, CHAN), F32)

    pass_two(last)

    def product(j):
        rows = pl.ds(pl.multiple_of(j * WIDE, WIDE), WIDE)
        w_load(j).wait()
        part = lax.dot_general(ing[...], w[rows, :], (((1,), (1,)), ((), ())), preferred_element_type=F32)
        pbuf[j] = part.astype(BF16)

    def y_copy(j, k):
        to = rem(y + k, NY)
        return remote(
            pbuf.at[j, pl.ds(pl.multiple_of(to * PAIR, PAIR), PAIR)],
            ybuf.at[j, y],
            ys_sem.at[j],
            yr_sem.at[j],
            {"y": to},
        )

    def y_send(j):
        for k in range(1, NY):
            y_copy(j, k).start()

    def produce(j):
        product(j)
        y_send(j - 1)

        @pl.when(j == NCH - 1)
        def _():
            y_send(j)

    product(0)

    @pl.loop(1, FIRST)
    def _(j):
        produce(j)


    def z_copy(j):
        return remote(zs.at[j], zr.at[j], zs_sem.at[j], zr_sem.at[j], {"zh": 1 - zh})

    mine = pl.multiple_of(zh * OWN, OWN)
    other = pl.multiple_of((1 - zh) * OWN, OWN)

    def xhat_of(j):
        cols = pl.ds(pl.multiple_of(j * WIDE, WIDE), WIDE)
        return hid[:, cols].astype(F32) * inv[:, 0:1]

    def gain_of(j):
        return gain[0:1, pl.ds(pl.multiple_of(j * WIDE, WIDE), WIDE)]

    def arrive(j):
        z_copy(j).wait_recv()
        normed = own[j] + zr[j].astype(F32)
        own[j] = normed
        both = normed * xhat_of(j)
        sums = jnp.sum(both, 0, keepdims=True)
        for i in range(PER):
            gbuf[j * PER + i, 0:1, :] = sums[:, i * 128 : (i + 1) * 128]
        both = both * gain_of(j)
        mean[...] += sum(both[:, i * 128 : (i + 1) * 128] for i in range(PER))

        @pl.loop(0, PER)
        def _(i):
            p = j * PER + i

            @pl.when(p != q)
            def _():
                remote(
                    gbuf.at[p, pl.ds(0, 1)], gr.at[q, pl.ds(0, 1)], small_s.at[2], small_r.at[2], plane_device(p)
                ).start()

            @pl.when(p == q)
            def _():
                gr[q, 0:1, :] = gbuf[p, 0:1, :]

    def forward(j):
        drain(ybuf.at[j, pl.ds(0, NY - 1)], yr_sem.at[j])
        ybuf[j, y] = pbuf[j, pl.ds(pl.multiple_of(y * PAIR, PAIR), PAIR), :]

        def total(start):
            return sum(ybuf[j, s, pl.ds(start, OWN), :].astype(F32) for s in range(NY))

        zs[j] = total(other).astype(BF16)
        own[j] = total(mine)
        z_copy(j).start()

    mean[...] = jnp.zeros_like(mean)
    pl.semaphore_wait(far.at[1], 2)

    @pl.loop(0, WINDOW)
    def _(j):
        forward(j)

        @pl.when(j + FIRST < NCH)
        def _():
            produce(j + FIRST)

    @pl.loop(FIRST + WINDOW, NCH)
    def _(j):
        produce(j)

    sums = [jnp.sum(tacc[k], 0, keepdims=True) for k in range(5)]
    for p in range(NLINE):
        for k in range(5):
            tpc[p, k : k + 1, :] = sums[k][:, p * 128 : (p + 1) * 128]
    tr[line, 0:5, :] = tpc[line, 0:5, :]

    loads[4].wait()
    loads[5].wait()

    def squares(j, total):
        cols = pl.ds(pl.multiple_of(j * WIDE, WIDE), WIDE)
        h = hid[:, cols].astype(F32)
        h = h * h
        return total + sum(h[:, i * 128 : (i + 1) * 128] for i in range(PER))

    square = lax.fori_loop(0, NCH, squares, jnp.zeros((OWN, 128), F32))
    rms = jnp.sqrt(jnp.sum(square, -1, keepdims=True) * (1.0 / DIM) + 1e-05)
    inv[...] = jnp.broadcast_to(1.0 / rms, (OWN, 128))

    def line_copy(k, src, dst, i):
        return remote(src, dst, small_s.at[i], small_r.at[i], line_device(rem(line + k, NLINE)))

    @pl.loop(1, NLINE)
    def _(k):
        line_copy(k, tpc.at[rem(line + k, NLINE), pl.ds(0, 5)], tr.at[line, pl.ds(0, 5)], 0).start()

    def near_sums():
        drain(tr.at[pl.ds(0, NLINE - 1), pl.ds(0, 5)], small_r.at[0])
        tn[rem(zl, GROUP), 0:5, :] = jnp.sum(tr[:, 0:5, :], 0)

        def near_copy(k):
            mine = tn.at[rem(zl, GROUP), pl.ds(0, 5)]
            to = zl - rem(zl, GROUP) + rem(zl + k, GROUP)
            return remote(mine, mine, small_s.at[1], small_r.at[1], {"zl": to})

        @pl.loop(1, GROUP)
        def _(k):
            near_copy(k).start()

    def far_sums():
        drain(tn.at[pl.ds(0, GROUP - 1), pl.ds(0, 5)], small_r.at[1])
        tz[zl // GROUP, 0:5, :] = jnp.sum(tn[:, 0:5, :], 0)

        def far_copy(k):
            mine = tz.at[zl // GROUP, pl.ds(0, 5)]
            return remote(mine, mine, small_s.at[6], small_r.at[6], {"zl": rem(zl + k * GROUP, NZL)})

        @pl.loop(1, NZL // GROUP)
        def _(k):
            far_copy(k).start()

    @pl.loop(WINDOW, NCH)
    def _(j):
        forward(j)

        arrive(j - WINDOW)

        @pl.when(j == NCH - 4)
        def _():
            near_sums()

        @pl.when(j == NCH - 1)
        def _():
            far_sums()

    @pl.loop(NCH - WINDOW, NCH)
    def _(j):
        arrive(j)

    drain(gr.at[pl.ds(0, NPLANE - 1), pl.ds(0, 1)], small_r.at[2])
    za[z, 0:1, :] = jnp.sum(gr[:, 0:1, :], 0)

    def z_share(k):
        remote(
            za.at[z, pl.ds(0, 1)], za.at[z, pl.ds(0, 1)], small_s.at[4], small_r.at[4], z_device(z + k)
        ).start()

    z_share(NZ // 2)

    @pl.loop(1, NZ // 2)
    def _(k):
        z_share(NZ // 2 - k)
        z_share(NZ // 2 + k)

    average = jnp.sum(mean[...], -1, keepdims=True) * (1.0 / DIM)

    @pl.loop(0, NCH)
    def _(j):
        cols = pl.ds(pl.multiple_of(j * WIDE, WIDE), WIDE)
        value = (gain_of(j) * own[j] - xhat_of(j) * average) * inv[:, 0:1]
        out_o[:, cols] = value.astype(BF16)

    drain(tz.at[pl.ds(0, NZL // GROUP - 1), pl.ds(0, 5)], small_r.at[6])
    tf[line, 0:5, :] = jnp.sum(tz[:, 0:5, :], 0)

    @pl.loop(1, NLINE)
    def _(k):
        line_copy(k, tf.at[line, pl.ds(0, 5)], tf.at[line, pl.ds(0, 5)], 3).start()

    drain(za.at[pl.ds(0, NZ - 1), pl.ds(0, 1)], small_r.at[4])
    ga[q, 0:1, :] = jnp.sum(za[:, 0:1, :], 0)

    @pl.loop(1, NPLANE)
    def _(k):
        remote(
            ga.at[q, pl.ds(0, 1)], ga.at[q, pl.ds(0, 1)], small_s.at[5], small_r.at[5], plane_device(rem(q + k, NPLANE))
        ).start()

    drain(tf.at[pl.ds(0, NLINE - 1), pl.ds(0, 5)], small_r.at[3])
    for p in range(NLINE):
        taps_o[:, p * 128 : (p + 1) * 128] = tf[p, 0:4, :]
        bias_o[:, p * 128 : (p + 1) * 128] = tf[p, 4:5, :]

    @pl.when(has_next)
    def _():
        to_next.wait_send()

    @pl.when(has_prev)
    def _():
        for copy in to_prev:
            copy.wait_send()

    @pl.loop(0, NCH)
    def _(j):
        drain(ybuf.at[j, pl.ds(0, NY - 1)], ys_sem.at[j])
        z_copy(j).wait_send()

    drain(tr.at[pl.ds(0, NLINE - 1), pl.ds(0, 5)], small_s.at[0])
    drain(tn.at[pl.ds(0, GROUP - 1), pl.ds(0, 5)], small_s.at[1])
    drain(tz.at[pl.ds(0, NZL // GROUP - 1), pl.ds(0, 5)], small_s.at[6])
    drain(gr.at[pl.ds(0, NPLANE - 1), pl.ds(0, 1)], small_s.at[2])
    drain(tf.at[pl.ds(0, NLINE - 1), pl.ds(0, 5)], small_s.at[3])
    drain(za.at[pl.ds(0, NZ - 1), pl.ds(0, 1)], small_s.at[4])
    drain(ga.at[pl.ds(0, NPLANE - 1), pl.ds(0, 1)], small_r.at[5])
    gain_o[...] = ga[:, 0, :]
    drain(ga.at[pl.ds(0, NPLANE - 1), pl.ds(0, 1)], small_s.at[5])


def hand_on(*arrays):
    count = len(arrays)

    def body(*refs):
        sem = refs[2 * count]
        copies = [pltpu.make_async_copy(refs[i], refs[count + i], sem.at[i]) for i in range(count)]
        for copy in copies:
            copy.start()
        for copy in copies:
            copy.wait()

    return pl.pallas_call(
        body,
        out_shape=tuple(jax.ShapeDtypeStruct(a.shape, a.dtype) for a in arrays),
        in_specs=[pl.BlockSpec(memory_space=pltpu.VMEM)] * count,
        out_specs=(pl.BlockSpec(memory_space=pltpu.HBM),) * count,
        scratch_shapes=[pltpu.SemaphoreType.DMA((count,))],
        compiler_params=pltpu.CompilerParams(vmem_limit_bytes=4 << 20),
        name="hand_on",
    )(*arrays)


def on_device(hidden_in, norm_gain, proj_weight, conv_in, conv_weight, conv_bias, act_grad):
    vmem = pltpu.VMEM
    dma = pltpu.SemaphoreType.DMA
    out, gain, taps, bias = pl.pallas_call(
        kernel,
        out_shape=(
            jax.ShapeDtypeStruct((OWN, DIM), BF16),
            jax.ShapeDtypeStruct((NPLANE, 128), F32),
            jax.ShapeDtypeStruct((4, CHAN), F32),
            jax.ShapeDtypeStruct((1, CHAN), F32),
        ),
        in_specs=[pl.BlockSpec(memory_space=pltpu.HBM)] * 7,
        out_specs=(pl.BlockSpec(memory_space=vmem),) * 4,
        scratch_shapes=[
            vmem((OWN, DIM), BF16),
            vmem((1, DIM), F32),
            vmem((DIM, CHAN), BF16),
            vmem((ROWS, CHAN), BF16),
            vmem((4, CHAN), F32),
            vmem((1, CHAN), F32),
            vmem((ROWS, CHAN), BF16),
            vmem((16, CHAN), BF16),
            vmem((16, CHAN), BF16),
            vmem((16, CHAN), BF16),
            vmem((ROWS + 16, CHAN), F32),
            vmem((ROWS + 8, CHAN), F32),
            vmem((ROWS, CHAN), BF16),
            vmem((5, 8, CHAN), F32),
            vmem((NCH, ROWS, WIDE), BF16),
            vmem((NCH, NY, PAIR, WIDE), BF16),
            vmem((NCH, OWN, WIDE), F32),
            vmem((NCH, OWN, WIDE), BF16),
            vmem((NCH, OWN, WIDE), BF16),
            vmem((OWN, 128), F32),
            vmem((OWN, 128), F32),
            vmem((NPLANE, 8, 128), F32),
            vmem((NPLANE, 8, 128), F32),
            vmem((NZ, 8, 128), F32),
            vmem((NPLANE, 8, 128), F32),
            vmem((NLINE, 8, 128), F32),
            vmem((NLINE, 8, 128), F32),
            vmem((GROUP, 8, 128), F32),
            vmem((NZL // GROUP, 8, 128), F32),
            vmem((NLINE, 8, 128), F32),
            dma((6,)),
            dma((NCH,)),
            dma((3,)),
            dma((3,)),
            dma((NCH,)),
            dma((NCH,)),
            dma((NCH,)),
            dma((NCH,)),
            dma((7,)),
            dma((7,)),
            pltpu.SemaphoreType.REGULAR((2,)),
        ],
        compiler_params=pltpu.CompilerParams(collective_id=0, has_side_effects=True, vmem_limit_bytes=40 << 20),
        name="layer_backward",
    )(
        *(
            pltpu.with_memory_space_constraint(a, pltpu.HBM)
            for a in (
                hidden_in,
                norm_gain.reshape(1, DIM),
                proj_weight,
                conv_in,
                conv_weight,
                conv_bias.reshape(1, CHAN),
                act_grad,
            )
        )
    )
    out, gain, taps, bias = hand_on(out, gain, taps, bias)
    return out, gain.reshape(DIM), taps, bias.reshape(CHAN)


def solution(mesh):
    finer = Mesh(mesh.devices.reshape(NZL, NX, NC, NY, NZH), ("zl", "x", "c", "y", "zh"))
    ctx = ("zl", "x", "c")
    tp = ("y", "zh")
    return jax.shard_map(
        on_device,
        mesh=finer,
        in_specs=(
            P(ctx + tp, None),
            P(),
            P(None, tp),
            P(ctx, tp),
            P(None, tp),
            P(tp),
            P(ctx, tp),
        ),
        out_specs=(P(ctx + tp, None), P(), P(None, tp), P(tp)),
        check_vma=False,
    )
```

```python
import jax
import jax.numpy as jnp
from jax import lax
from jax.experimental import pallas as pl
from jax.experimental.pallas import tpu as pltpu
from jax.sharding import Mesh
from jax.sharding import PartitionSpec as P

MESH = pl.DeviceIdType.MESH
NZL, NX, NC, NY, NZH = 16, 4, 2, 4, 2
NZ = NZL * NZH
NPLANE = NX * NC * NY
NLINE = NX * NC
NCTX = NZL * NX * NC
ROWS = 256
CHAN = 1024
DIM = 4096
NCH = 16
WIDE = DIM // NCH
PER = WIDE // 128
OWN = 32
PAIR = 64
TILE = 16
NEAR = 4
AROUND = NY - 1 + NX - 1 + NC - 1
WINDOW = 8
FIRST = 10
WLOADS = 4
GROUP = 4
F32 = jnp.float32
CHIPS = sorted(
    ((i, j) for i in range(NX) for j in range(NY)), key=lambda p: -min(p[0], NX - p[0]) - min(p[1], NY - p[1])
)
CHIP_X = sum(p[0] << (2 * i) for i, p in enumerate(CHIPS))
CHIP_Y = sum(p[1] << (2 * i) for i, p in enumerate(CHIPS))
BF16 = jnp.bfloat16


def rem(a, b):
    return lax.rem(a, b)


def z_device(z):
    z = rem(z, NZ)
    return {"zh": z // NZL, "zl": rem(z, NZL)}


def plane_device(q):
    return {"x": q // (NY * NC), "y": rem(q // NC, NY), "c": rem(q, NC)}


def packed(table, i):
    signed = table - (1 << 32) if table >> 31 else table
    return lax.shift_right_logical(jnp.int32(signed), 2 * i) & 3


def chip_at(place, core):
    return {"x": packed(CHIP_X, place), "y": packed(CHIP_Y, place), "c": core}


def line_device(q):
    return {"x": q // NC, "c": rem(q, NC)}


def ctx_device(n):
    return {"zl": n // NLINE, "x": rem(n // NC, NX), "c": rem(n, NC)}


def kernel(
    hid_h, gain_h, w_h, conv_h, cw_h, cb_h, act_h,
    out_o, gain_o, taps_o, bias_o,
    hid, gain, w, conv, cw, cb, act,
    hprev, hconv, hact,
    xf, pg, ing, tacc,
    pbuf, ybuf, own, zs, zr, inv, mean,
    gbuf, gr, za, ga, tpc, tr, tn, tz, tf,
    in_sem, w_sem, hs_sem, hr_sem, ys_sem, yr_sem, zs_sem, zr_sem, small_s, small_r, far,
):
    zl = lax.axis_index("zl")
    zh = lax.axis_index("zh")
    x = lax.axis_index("x")
    y = lax.axis_index("y")
    c = lax.axis_index("c")
    z = zh * NZL + zl
    q = (x * NY + y) * NC + c
    line = x * NC + c
    place = sum(jnp.where(jnp.logical_and(x == a, y == b), i, 0) for i, (a, b) in enumerate(CHIPS))
    owner = c == NC - 1
    n = zl * NLINE + line
    has_next = n < NCTX - 1
    has_prev = n > 0
    chip_next = jnp.logical_and(c == NC - 1, has_next)
    chip_prev = jnp.logical_and(c == 0, has_prev)

    def remote(src, dst, send, recv, device):
        return pltpu.make_async_remote_copy(
            src_ref=src, dst_ref=dst, send_sem=send, recv_sem=recv, device_id=device, device_id_type=MESH
        )

    def drain(ref, sem):
        pltpu.make_async_copy(ref, ref, sem).wait()

    loads = [
        pltpu.make_async_copy(a, b, in_sem.at[i])
        for i, (a, b) in enumerate(
            [
                (conv_h, conv),
                (act_h, act),
                (cw_h, cw),
                (cb_h, cb),
                (hid_h, hid),
                (gain_h, gain),
            ]
        )
    ]
    for load in loads[:4]:
        load.start()

    barrier = pltpu.get_barrier_semaphore()

    def greet(device):
        pl.semaphore_signal(barrier, 1, device_id=device, device_id_type=MESH)

    def plane_neighbours(visit):
        for k in (2, 1, 3):
            visit({"y": rem(y + k, NY)})
            visit({"x": rem(x + k, NX)})
        visit({"c": 1 - c})

    @pl.loop(0, NEAR)
    def _(k):
        greet(z_device(z + (NEAR - k)))
        greet(z_device(z + NZ - (NEAR - k)))

    plane_neighbours(greet)

    @pl.when(chip_next)
    def _():
        greet(ctx_device(n + 1))

    @pl.when(chip_prev)
    def _():
        greet(ctx_device(n - 1))

    for load in loads[4:]:
        load.start()

    def w_load(i):
        rows = pl.ds(pl.multiple_of(i * (DIM // WLOADS), DIM // WLOADS), DIM // WLOADS)
        return pltpu.make_async_copy(w_h.at[rows], w.at[rows], w_sem.at[i])

    @pl.loop(0, WLOADS)
    def _(i):
        w_load(i).start()

    xf[0:8, :] = jnp.zeros((8, CHAN), F32)
    tacc[...] = jnp.zeros_like(tacc)
    loads[0].wait()

    @pl.loop(0, ROWS // TILE)
    def _(i):
        t = pl.multiple_of(i * TILE, TILE)
        xf[pl.ds(t + 8, TILE), :] = conv[pl.ds(t, TILE), :].astype(F32)

    for load in loads[1:4]:
        load.wait()

    def grad_tile(t, rows, cotangent):
        above = xf[pl.ds(t, rows + 8), :]
        xs = [above[8 - k : 8 - k + rows] for k in range(4)]
        pre = cb[0:1, :] + sum(cw[k : k + 1, :] * xs[k] for k in range(4))
        s = 1.0 / (1.0 + jnp.exp(-pre))
        return cotangent * s * (1.0 + pre * (1.0 - s)), xs

    def pass_one(i):
        t = pl.multiple_of(i * TILE, TILE)
        g, xs = grad_tile(t, TILE, act[pl.ds(t, TILE), :].astype(F32))
        pg[pl.ds(t, TILE), :] = g
        for k in range(5):
            term = g * xs[k] if k < 4 else g
            tacc[k] += term[0:8] + term[8:16]

    def pass_two(i):
        t = pl.multiple_of(i * TILE, TILE)
        below = pg[pl.ds(t, TILE + 8), :]
        total = sum(cw[k : k + 1, :] * below[k : k + TILE] for k in range(4))
        ing[pl.ds(t, TILE), :] = total.astype(BF16)

    last = ROWS // TILE - 1

    @pl.loop(1, last + 1)
    def _(i):
        pass_one(i)

    pl.semaphore_wait(
        barrier,
        AROUND + 2 * NEAR + jnp.where(chip_next, 1, 0) + jnp.where(chip_prev, 1, 0),
    )
    for step in (NEAR, NZ - NEAR):
        pl.semaphore_signal(far.at[0], 1, device_id=z_device(z + step), device_id_type=MESH)

    to_next = remote(conv.at[pl.ds(ROWS - 16, 16)], hprev, hs_sem.at[0], hr_sem.at[0], ctx_device(jnp.minimum(n + 1, NCTX - 1)))
    to_prev = [
        remote(conv.at[pl.ds(0, 16)], hconv, hs_sem.at[1], hr_sem.at[1], ctx_device(jnp.maximum(n - 1, 0))),
        remote(act.at[pl.ds(0, 16)], hact, hs_sem.at[2], hr_sem.at[2], ctx_device(jnp.maximum(n - 1, 0))),
    ]

    @pl.when(has_next)
    def _():
        to_next.start()

    @pl.when(has_prev)
    def _():
        for copy in to_prev:
            copy.start()

    plane_neighbours(lambda device: pl.semaphore_signal(far.at[2], 1, device_id=device, device_id_type=MESH))

    @pl.loop(1, last)
    def _(i):
        pass_two(i)

    loads[4].wait()
    loads[5].wait()

    def squares(j, total):
        cols = pl.ds(pl.multiple_of(j * WIDE, WIDE), WIDE)
        h = hid[:, cols].astype(F32)
        h = h * h
        return total + sum(h[:, i * 128 : (i + 1) * 128] for i in range(PER))

    square = lax.fori_loop(0, NCH, squares, jnp.zeros((OWN, 128), F32))
    rms = jnp.sqrt(jnp.sum(square, -1, keepdims=True) * (1.0 / DIM) + 1e-05)
    inv[...] = jnp.broadcast_to(1.0 / rms, (OWN, 128))
    pl.semaphore_wait(far.at[0], 2)
    for step in (2 * NEAR, NZ - 2 * NEAR):
        pl.semaphore_signal(far.at[1], 1, device_id=z_device(z + step), device_id_type=MESH)

    @pl.when(has_prev)
    def _():
        to_next.wait_recv()
        xf[0:8, :] = hprev[8:16, :].astype(F32)

    pass_one(0)
    pass_two(0)

    @pl.when(has_next)
    def _():
        for copy in to_prev:
            copy.wait_recv()
        xf[ROWS + 8 : ROWS + 16, :] = hconv[0:8, :].astype(F32)
        g, _ = grad_tile(ROWS, 8, hact[0:8, :].astype(F32))
        pg[ROWS : ROWS + 8, :] = g

    @pl.when(jnp.logical_not(has_next))
    def _():
        pg[ROWS : ROWS + 8, :] = jnp.zeros((8, CHAN), F32)

    pass_two(last)

    def product(j):
        rows = pl.ds(pl.multiple_of(j * WIDE, WIDE), WIDE)

        @pl.when(rem(j, NCH // WLOADS) == 0)
        def _():
            w_load(j // (NCH // WLOADS)).wait()

        part = lax.dot_general(ing[...], w[rows, :], (((1,), (1,)), ((), ())), preferred_element_type=F32)
        pbuf[j] = part.astype(BF16)

    def y_copy(j, k):
        to = rem(y + k, NY)
        return remote(
            pbuf.at[j, pl.ds(pl.multiple_of(to * PAIR, PAIR), PAIR)],
            ybuf.at[j, y],
            ys_sem,
            yr_sem.at[j],
            {"y": to},
        )

    def y_send(j):
        for k in range(1, NY):
            y_copy(j, k).start()

    def produce(j):
        product(j)
        y_send(j - 1)

        @pl.when(j == NCH - 1)
        def _():
            y_send(j)

    product(0)

    @pl.loop(1, FIRST)
    def _(j):
        produce(j)


    def z_copy(j):
        return remote(zs.at[j], zr.at[j], zs_sem, zr_sem.at[j], {"zh": 1 - zh})

    mine = pl.multiple_of(zh * OWN, OWN)
    other = pl.multiple_of((1 - zh) * OWN, OWN)

    def xhat_of(j):
        cols = pl.ds(pl.multiple_of(j * WIDE, WIDE), WIDE)
        return hid[:, cols].astype(F32) * inv[:, 0:1]

    def gain_of(j):
        return gain[0:1, pl.ds(pl.multiple_of(j * WIDE, WIDE), WIDE)]

    def share(j, sums):
        for i in range(PER):
            gbuf[j, i : i + 1, :] = sums[:, i * 128 : (i + 1) * 128]

    def share_send(j):
        mine = jnp.logical_and(j == place, owner)

        @pl.when(jnp.logical_not(mine))
        def _():
            remote(
                gbuf.at[j, pl.ds(0, PER)],
                gr.at[q, pl.ds(0, PER)],
                small_s.at[2],
                small_r.at[2],
                chip_at(j, NC - 1),
            ).start()

        @pl.when(mine)
        def _():
            gr[q, 0:PER, :] = gbuf[j, 0:PER, :]

    def arrive(j):
        z_copy(j).wait_recv()
        normed = own[j] + zr[j].astype(F32)
        own[j] = normed
        both = normed * xhat_of(j)
        share(j, jnp.sum(both, 0, keepdims=True))
        both = both * gain_of(j)
        mean[...] += sum(both[:, i * 128 : (i + 1) * 128] for i in range(PER))
        share_send(j)

        @pl.when(j == 3)
        def _():
            near_sums()

        @pl.when(j == 10)
        def _():
            far_sums()

    def forward(j):
        drain(ybuf.at[j, pl.ds(0, NY - 1)], yr_sem.at[j])
        ybuf[j, y] = pbuf[j, pl.ds(pl.multiple_of(y * PAIR, PAIR), PAIR), :]

        def total(start):
            return sum(ybuf[j, s, pl.ds(start, OWN), :].astype(F32) for s in range(NY))

        zs[j] = total(other).astype(BF16)
        own[j] = total(mine)
        z_copy(j).start()

    mean[...] = jnp.zeros_like(mean)
    pl.semaphore_wait(far.at[1], 2)

    @pl.loop(0, WINDOW)
    def _(j):
        forward(j)

        @pl.when(j + FIRST < NCH)
        def _():
            produce(j + FIRST)

    pl.semaphore_wait(far.at[2], AROUND)
    plane_neighbours(lambda device: pl.semaphore_signal(far.at[3], 1, device_id=device, device_id_type=MESH))

    sums = [jnp.sum(tacc[k], 0, keepdims=True) for k in range(5)]
    for p in range(NLINE):
        for k in range(5):
            tpc[p, k : k + 1, :] = sums[k][:, p * 128 : (p + 1) * 128]
    tr[line, 0:5, :] = tpc[line, 0:5, :]

    def line_copy(k, src, dst, i):
        return remote(src, dst, small_s.at[i], small_r.at[i], line_device(rem(line + k, NLINE)))

    @pl.loop(1, NLINE)
    def _(k):
        line_copy(k, tpc.at[rem(line + k, NLINE), pl.ds(0, 5)], tr.at[line, pl.ds(0, 5)], 0).start()

    def near_sums():
        drain(tr.at[pl.ds(0, NLINE - 1), pl.ds(0, 5)], small_r.at[0])
        tn[rem(zl, GROUP), 0:5, :] = jnp.sum(tr[:, 0:5, :], 0)

        def near_copy(k):
            mine = tn.at[rem(zl, GROUP), pl.ds(0, 5)]
            to = zl - rem(zl, GROUP) + rem(zl + k, GROUP)
            return remote(mine, mine, small_s.at[1], small_r.at[1], {"zl": to})

        @pl.loop(1, GROUP)
        def _(k):
            near_copy(k).start()

    def far_sums():
        drain(tn.at[pl.ds(0, GROUP - 1), pl.ds(0, 5)], small_r.at[1])
        tz[zl // GROUP, 0:5, :] = jnp.sum(tn[:, 0:5, :], 0)

        def far_copy(k):
            mine = tz.at[zl // GROUP, pl.ds(0, 5)]
            return remote(mine, mine, small_s.at[6], small_r.at[6], {"zl": rem(zl + k * GROUP, NZL)})

        @pl.loop(1, NZL // GROUP)
        def _(k):
            far_copy(k).start()

    pl.semaphore_wait(far.at[3], AROUND)

    @pl.loop(WINDOW, NCH)
    def _(j):
        forward(j)
        arrive(j - WINDOW)

    @pl.loop(NCH - WINDOW, NCH)
    def _(j):
        arrive(j)

    @pl.when(owner)
    def _():
        drain(gr.at[pl.ds(0, NPLANE - 1), pl.ds(0, PER)], small_r.at[2])
        za[z, 0:PER, :] = jnp.sum(gr[:, 0:PER, :], 0)

        def z_share(k):
            mine = za.at[z, pl.ds(0, PER)]
            remote(mine, mine, small_s.at[4], small_r.at[4], z_device(z + k)).start()

        z_share(NZ // 2)

        @pl.loop(1, NZ // 2)
        def _(k):
            z_share(NZ // 2 - k)
            z_share(NZ // 2 + k)

    average = jnp.sum(mean[...], -1, keepdims=True) * (1.0 / DIM)

    @pl.loop(0, NCH)
    def _(j):
        cols = pl.ds(pl.multiple_of(j * WIDE, WIDE), WIDE)
        value = (gain_of(j) * own[j] - xhat_of(j) * average) * inv[:, 0:1]
        out_o[:, cols] = value.astype(BF16)

    drain(tz.at[pl.ds(0, NZL // GROUP - 1), pl.ds(0, 5)], small_r.at[6])
    tf[line, 0:5, :] = jnp.sum(tz[:, 0:5, :], 0)

    @pl.loop(1, NLINE)
    def _(k):
        line_copy(k, tf.at[line, pl.ds(0, 5)], tf.at[line, pl.ds(0, 5)], 3).start()

    @pl.when(owner)
    def _():
        drain(za.at[pl.ds(0, NZ - 1), pl.ds(0, PER)], small_r.at[4])
        ga[place, 0:PER, :] = jnp.sum(za[:, 0:PER, :], 0)

        @pl.loop(0, NPLANE)
        def _(k):
            to = NPLANE - 1 - k

            @pl.when(to != place * NC + c)
            def _():
                mine = ga.at[place, pl.ds(0, PER)]
                remote(mine, mine, small_s.at[5], small_r.at[5], chip_at(to // NC, rem(to, NC))).start()

    drain(tf.at[pl.ds(0, NLINE - 1), pl.ds(0, 5)], small_r.at[3])
    for p in range(NLINE):
        taps_o[:, p * 128 : (p + 1) * 128] = tf[p, 0:4, :]
        bias_o[:, p * 128 : (p + 1) * 128] = tf[p, 4:5, :]

    @pl.when(has_next)
    def _():
        to_next.wait_send()

    @pl.when(has_prev)
    def _():
        for copy in to_prev:
            copy.wait_send()

    drain(ybuf.at[:, pl.ds(0, NY - 1)], ys_sem)
    drain(zs, zs_sem)
    drain(tr.at[pl.ds(0, NLINE - 1), pl.ds(0, 5)], small_s.at[0])
    drain(tn.at[pl.ds(0, GROUP - 1), pl.ds(0, 5)], small_s.at[1])
    drain(tz.at[pl.ds(0, NZL // GROUP - 1), pl.ds(0, 5)], small_s.at[6])
    drain(tf.at[pl.ds(0, NLINE - 1), pl.ds(0, 5)], small_s.at[3])

    @pl.when(owner)
    def _():
        drain(gr.at[pl.ds(0, NCH - 1), pl.ds(0, PER)], small_s.at[2])
        drain(za.at[pl.ds(0, NZ - 1), pl.ds(0, PER)], small_s.at[4])
        drain(ga.at[pl.ds(0, NCH - 1), pl.ds(0, PER)], small_r.at[5])

    @pl.when(jnp.logical_not(owner))
    def _():
        drain(gr.at[pl.ds(0, NCH), pl.ds(0, PER)], small_s.at[2])
        drain(ga.at[pl.ds(0, NCH), pl.ds(0, PER)], small_r.at[5])

    gain_o[...] = ga[:, 0:PER, :]

    @pl.when(owner)
    def _():
        drain(gr.at[pl.ds(0, NPLANE - 1), pl.ds(0, PER)], small_s.at[5])


def hand_on(*arrays):
    count = len(arrays)

    def body(*refs):
        sem = refs[2 * count]
        copies = [pltpu.make_async_copy(refs[i], refs[count + i], sem.at[i]) for i in range(count)]
        for copy in copies:
            copy.start()
        for copy in copies:
            copy.wait()

    return pl.pallas_call(
        body,
        out_shape=tuple(jax.ShapeDtypeStruct(a.shape, a.dtype) for a in arrays),
        in_specs=[pl.BlockSpec(memory_space=pltpu.VMEM)] * count,
        out_specs=(pl.BlockSpec(memory_space=pltpu.HBM),) * count,
        scratch_shapes=[pltpu.SemaphoreType.DMA((count,))],
        compiler_params=pltpu.CompilerParams(vmem_limit_bytes=4 << 20),
        name="hand_on",
    )(*arrays)


def on_device(hidden_in, norm_gain, proj_weight, conv_in, conv_weight, conv_bias, act_grad):
    vmem = pltpu.VMEM
    dma = pltpu.SemaphoreType.DMA
    out, gain, taps, bias = pl.pallas_call(
        kernel,
        out_shape=(
            jax.ShapeDtypeStruct((OWN, DIM), BF16),
            jax.ShapeDtypeStruct((NCH, PER, 128), F32),
            jax.ShapeDtypeStruct((4, CHAN), F32),
            jax.ShapeDtypeStruct((1, CHAN), F32),
        ),
        in_specs=[pl.BlockSpec(memory_space=pltpu.HBM)] * 7,
        out_specs=(pl.BlockSpec(memory_space=vmem),) * 4,
        scratch_shapes=[
            vmem((OWN, DIM), BF16),
            vmem((1, DIM), F32),
            vmem((DIM, CHAN), BF16),
            vmem((ROWS, CHAN), BF16),
            vmem((4, CHAN), F32),
            vmem((1, CHAN), F32),
            vmem((ROWS, CHAN), BF16),
            vmem((16, CHAN), BF16),
            vmem((16, CHAN), BF16),
            vmem((16, CHAN), BF16),
            vmem((ROWS + 16, CHAN), F32),
            vmem((ROWS + 8, CHAN), F32),
            vmem((ROWS, CHAN), BF16),
            vmem((5, 8, CHAN), F32),
            vmem((NCH, ROWS, WIDE), BF16),
            vmem((NCH, NY, PAIR, WIDE), BF16),
            vmem((NCH, OWN, WIDE), F32),
            vmem((NCH, OWN, WIDE), BF16),
            vmem((NCH, OWN, WIDE), BF16),
            vmem((OWN, 128), F32),
            vmem((OWN, 128), F32),
            vmem((NCH, 8, 128), F32),
            vmem((NPLANE, 8, 128), F32),
            vmem((NZ, 8, 128), F32),
            vmem((NCH, 8, 128), F32),
            vmem((NLINE, 8, 128), F32),
            vmem((NLINE, 8, 128), F32),
            vmem((GROUP, 8, 128), F32),
            vmem((NZL // GROUP, 8, 128), F32),
            vmem((NLINE, 8, 128), F32),
            dma((6,)),
            dma((WLOADS,)),
            dma((3,)),
            dma((3,)),
            dma,
            dma((NCH,)),
            dma,
            dma((NCH,)),
            dma((7,)),
            dma((7,)),
            pltpu.SemaphoreType.REGULAR((4,)),
        ],
        compiler_params=pltpu.CompilerParams(collective_id=0, has_side_effects=True, vmem_limit_bytes=40 << 20),
        name="layer_backward",
    )(
        *(
            pltpu.with_memory_space_constraint(a, pltpu.HBM)
            for a in (
                hidden_in,
                norm_gain.reshape(1, DIM),
                proj_weight,
                conv_in,
                conv_weight,
                conv_bias.reshape(1, CHAN),
                act_grad,
            )
        )
    )
    out, gain, taps, bias = hand_on(out, gain, taps, bias)
    return out, gain.reshape(DIM), taps, bias.reshape(CHAN)


def solution(mesh):
    finer = Mesh(mesh.devices.reshape(NZL, NX, NC, NY, NZH), ("zl", "x", "c", "y", "zh"))
    ctx = ("zl", "x", "c")
    tp = ("y", "zh")
    return jax.shard_map(
        on_device,
        mesh=finer,
        in_specs=(
            P(ctx + tp, None),
            P(),
            P(None, tp),
            P(ctx, tp),
            P(None, tp),
            P(tp),
            P(ctx, tp),
        ),
        out_specs=(P(ctx + tp, None), P(), P(None, tp), P(tp)),
        check_vma=False,
    )
```

```python
import jax
import jax.numpy as jnp
from jax import lax
from jax.experimental import pallas as pl
from jax.experimental.pallas import tpu as pltpu
from jax.sharding import Mesh
from jax.sharding import PartitionSpec as P

MESH = pl.DeviceIdType.MESH
NZL, NX, NC, NY, NZH = 16, 4, 2, 4, 2
NZ = NZL * NZH
NPLANE = NX * NC * NY
NLINE = NX * NC
NCTX = NZL * NX * NC
ROWS = 256
CHAN = 1024
DIM = 4096
NCH = 16
WIDE = DIM // NCH
PER = WIDE // 128
OWN = 32
PAIR = 64
TILE = 16
NEAR = 4
AROUND = NY - 1 + NX - 1 + NC - 1
WINDOW = 9
FIRST = 7
EXTRA = 3
WLOADS = 4
GROUP = 4
F32 = jnp.float32
CHIPS = sorted(
    ((i, j) for i in range(NX) for j in range(NY)), key=lambda p: -min(p[0], NX - p[0]) - min(p[1], NY - p[1])
)
CHIP_X = sum(p[0] << (2 * i) for i, p in enumerate(CHIPS))
CHIP_Y = sum(p[1] << (2 * i) for i, p in enumerate(CHIPS))
BF16 = jnp.bfloat16


def rem(a, b):
    return lax.rem(a, b)


def z_device(z):
    z = rem(z, NZ)
    return {"zh": z // NZL, "zl": rem(z, NZL)}


def plane_device(q):
    return {"x": q // (NY * NC), "y": rem(q // NC, NY), "c": rem(q, NC)}


def packed(table, i):
    signed = table - (1 << 32) if table >> 31 else table
    return lax.shift_right_logical(jnp.int32(signed), 2 * i) & 3


def chip_at(place, core):
    return {"x": packed(CHIP_X, place), "y": packed(CHIP_Y, place), "c": core}


def line_device(q):
    return {"x": q // NC, "c": rem(q, NC)}


def ctx_device(n):
    return {"zl": n // NLINE, "x": rem(n // NC, NX), "c": rem(n, NC)}


def kernel(
    hid_h, gain_h, w_h, conv_h, cw_h, cb_h, act_h,
    out_o, gain_o, taps_o, bias_o,
    hid, gain, w, conv, cw, cb, act,
    hprev, hconv, hact,
    xf, pg, ing, tacc,
    pbuf, ybuf, own, zs, zr, inv, mean,
    gbuf, gr, za, ga, tpc, tr, tn, tz, tf,
    in_sem, w_sem, hs_sem, hr_sem, ys_sem, yr_sem, zs_sem, zr_sem, small_s, small_r, far,
):
    zl = lax.axis_index("zl")
    zh = lax.axis_index("zh")
    x = lax.axis_index("x")
    y = lax.axis_index("y")
    c = lax.axis_index("c")
    z = zh * NZL + zl
    q = (x * NY + y) * NC + c
    line = x * NC + c
    place = sum(jnp.where(jnp.logical_and(x == a, y == b), i, 0) for i, (a, b) in enumerate(CHIPS))
    owner = c == NC - 1
    ahead = WINDOW + EXTRA * (1 - c)
    n = zl * NLINE + line
    has_next = n < NCTX - 1
    has_prev = n > 0
    chip_next = jnp.logical_and(c == NC - 1, has_next)
    chip_prev = jnp.logical_and(c == 0, has_prev)

    def remote(src, dst, send, recv, device):
        return pltpu.make_async_remote_copy(
            src_ref=src, dst_ref=dst, send_sem=send, recv_sem=recv, device_id=device, device_id_type=MESH
        )

    def drain(ref, sem):
        pltpu.make_async_copy(ref, ref, sem).wait()

    loads = [
        pltpu.make_async_copy(a, b, in_sem.at[i])
        for i, (a, b) in enumerate(
            [
                (conv_h, conv),
                (act_h, act),
                (cw_h, cw),
                (cb_h, cb),
                (hid_h, hid),
                (gain_h, gain),
            ]
        )
    ]
    for load in loads[:4]:
        load.start()

    barrier = pltpu.get_barrier_semaphore()

    def greet(device):
        pl.semaphore_signal(barrier, 1, device_id=device, device_id_type=MESH)

    def plane_neighbours(visit):
        for k in (2, 1, 3):
            visit({"y": rem(y + k, NY)})
            visit({"x": rem(x + k, NX)})
        visit({"c": 1 - c})

    @pl.loop(0, NEAR)
    def _(k):
        greet(z_device(z + (NEAR - k)))
        greet(z_device(z + NZ - (NEAR - k)))

    plane_neighbours(greet)

    @pl.when(chip_next)
    def _():
        greet(ctx_device(n + 1))

    @pl.when(chip_prev)
    def _():
        greet(ctx_device(n - 1))

    for load in loads[4:]:
        load.start()

    def w_load(i):
        rows = pl.ds(pl.multiple_of(i * (DIM // WLOADS), DIM // WLOADS), DIM // WLOADS)
        return pltpu.make_async_copy(w_h.at[rows], w.at[rows], w_sem.at[i])

    @pl.loop(0, WLOADS)
    def _(i):
        w_load(i).start()

    xf[0:8, :] = jnp.zeros((8, CHAN), F32)
    tacc[...] = jnp.zeros_like(tacc)
    loads[0].wait()

    @pl.loop(0, ROWS // TILE)
    def _(i):
        t = pl.multiple_of(i * TILE, TILE)
        xf[pl.ds(t + 8, TILE), :] = conv[pl.ds(t, TILE), :].astype(F32)

    for load in loads[1:4]:
        load.wait()

    def grad_tile(t, rows, cotangent):
        above = xf[pl.ds(t, rows + 8), :]
        xs = [above[8 - k : 8 - k + rows] for k in range(4)]
        pre = cb[0:1, :] + sum(cw[k : k + 1, :] * xs[k] for k in range(4))
        s = 1.0 / (1.0 + jnp.exp(-pre))
        return cotangent * s * (1.0 + pre * (1.0 - s)), xs

    def pass_one(i):
        t = pl.multiple_of(i * TILE, TILE)
        g, xs = grad_tile(t, TILE, act[pl.ds(t, TILE), :].astype(F32))
        pg[pl.ds(t, TILE), :] = g
        for k in range(5):
            term = g * xs[k] if k < 4 else g
            tacc[k] += term[0:8] + term[8:16]

    def pass_two(i):
        t = pl.multiple_of(i * TILE, TILE)
        below = pg[pl.ds(t, TILE + 8), :]
        total = sum(cw[k : k + 1, :] * below[k : k + TILE] for k in range(4))
        ing[pl.ds(t, TILE), :] = total.astype(BF16)

    last = ROWS // TILE - 1

    @pl.loop(1, last + 1)
    def _(i):
        pass_one(i)

    pl.semaphore_wait(
        barrier,
        AROUND + 2 * NEAR + jnp.where(chip_next, 1, 0) + jnp.where(chip_prev, 1, 0),
    )
    for step in (NEAR, NZ - NEAR):
        pl.semaphore_signal(far.at[0], 1, device_id=z_device(z + step), device_id_type=MESH)

    to_next = remote(conv.at[pl.ds(ROWS - 16, 16)], hprev, hs_sem.at[0], hr_sem.at[0], ctx_device(jnp.minimum(n + 1, NCTX - 1)))
    to_prev = [
        remote(conv.at[pl.ds(0, 16)], hconv, hs_sem.at[1], hr_sem.at[1], ctx_device(jnp.maximum(n - 1, 0))),
        remote(act.at[pl.ds(0, 16)], hact, hs_sem.at[2], hr_sem.at[2], ctx_device(jnp.maximum(n - 1, 0))),
    ]

    @pl.when(has_next)
    def _():
        to_next.start()

    @pl.when(has_prev)
    def _():
        for copy in to_prev:
            copy.start()

    plane_neighbours(lambda device: pl.semaphore_signal(far.at[2], 1, device_id=device, device_id_type=MESH))

    @pl.loop(1, last)
    def _(i):
        pass_two(i)

    loads[4].wait()
    loads[5].wait()

    def squares(j, total):
        cols = pl.ds(pl.multiple_of(j * WIDE, WIDE), WIDE)
        h = hid[:, cols].astype(F32)
        h = h * h
        return total + sum(h[:, i * 128 : (i + 1) * 128] for i in range(PER))

    square = lax.fori_loop(0, NCH, squares, jnp.zeros((OWN, 128), F32))
    rms = jnp.sqrt(jnp.sum(square, -1, keepdims=True) * (1.0 / DIM) + 1e-05)
    inv[...] = jnp.broadcast_to(1.0 / rms, (OWN, 128))
    pl.semaphore_wait(far.at[0], 2)
    for step in (2 * NEAR, NZ - 2 * NEAR):
        pl.semaphore_signal(far.at[1], 1, device_id=z_device(z + step), device_id_type=MESH)

    @pl.when(has_prev)
    def _():
        to_next.wait_recv()
        xf[0:8, :] = hprev[8:16, :].astype(F32)

    pass_one(0)
    pass_two(0)

    @pl.when(has_next)
    def _():
        for copy in to_prev:
            copy.wait_recv()
        xf[ROWS + 8 : ROWS + 16, :] = hconv[0:8, :].astype(F32)
        g, _ = grad_tile(ROWS, 8, hact[0:8, :].astype(F32))
        pg[ROWS : ROWS + 8, :] = g

    @pl.when(jnp.logical_not(has_next))
    def _():
        pg[ROWS : ROWS + 8, :] = jnp.zeros((8, CHAN), F32)

    pass_two(last)

    def product(j):
        rows = pl.ds(pl.multiple_of(j * WIDE, WIDE), WIDE)

        @pl.when(rem(j, NCH // WLOADS) == 0)
        def _():
            w_load(j // (NCH // WLOADS)).wait()

        part = lax.dot_general(ing[...], w[rows, :], (((1,), (1,)), ((), ())), preferred_element_type=F32)
        pbuf[j] = part.astype(BF16)

    def y_copy(j, k):
        to = rem(y + k, NY)
        return remote(
            pbuf.at[j, pl.ds(pl.multiple_of(to * PAIR, PAIR), PAIR)],
            ybuf.at[j, y],
            ys_sem,
            yr_sem.at[j],
            {"y": to},
        )

    def y_send(j):
        for k in range(1, NY):
            y_copy(j, k).start()

    def produce(j):
        product(j)
        y_send(j - 1)

        @pl.when(j == NCH - 1)
        def _():
            y_send(j)

    product(0)

    @pl.loop(1, FIRST)
    def _(j):
        produce(j)


    def z_copy(j):
        return remote(zs.at[j], zr.at[j], zs_sem, zr_sem.at[j], {"zh": 1 - zh})

    mine = pl.multiple_of(zh * OWN, OWN)
    other = pl.multiple_of((1 - zh) * OWN, OWN)

    def xhat_of(j):
        cols = pl.ds(pl.multiple_of(j * WIDE, WIDE), WIDE)
        return hid[:, cols].astype(F32) * inv[:, 0:1]

    def gain_of(j):
        return gain[0:1, pl.ds(pl.multiple_of(j * WIDE, WIDE), WIDE)]

    def share(j, sums):
        for i in range(PER):
            gbuf[j, i : i + 1, :] = sums[:, i * 128 : (i + 1) * 128]

    def share_send(j):
        mine = jnp.logical_and(j == place, owner)

        @pl.when(jnp.logical_not(mine))
        def _():
            remote(
                gbuf.at[j, pl.ds(0, PER)],
                gr.at[q, pl.ds(0, PER)],
                small_s.at[2],
                small_r.at[2],
                chip_at(j, NC - 1),
            ).start()

        @pl.when(mine)
        def _():
            gr[q, 0:PER, :] = gbuf[j, 0:PER, :]

    def arrive(j):
        z_copy(j).wait_recv()
        normed = own[j] + zr[j].astype(F32)
        own[j] = normed
        both = normed * xhat_of(j)
        share(j, jnp.sum(both, 0, keepdims=True))
        both = both * gain_of(j)
        mean[...] += sum(both[:, i * 128 : (i + 1) * 128] for i in range(PER))
        share_send(j)

        @pl.when(j == 3)
        def _():
            near_sums()

        @pl.when(j == 10)
        def _():
            far_sums()

    def forward(j):
        drain(ybuf.at[j, pl.ds(0, NY - 1)], yr_sem.at[j])
        ybuf[j, y] = pbuf[j, pl.ds(pl.multiple_of(y * PAIR, PAIR), PAIR), :]

        def total(start):
            return sum(ybuf[j, s, pl.ds(start, OWN), :].astype(F32) for s in range(NY))

        zs[j] = total(other).astype(BF16)
        own[j] = total(mine)
        z_copy(j).start()

    mean[...] = jnp.zeros_like(mean)
    pl.semaphore_wait(far.at[1], 2)

    @pl.loop(0, ahead)
    def _(j):
        forward(j)

        @pl.when(j + FIRST < NCH)
        def _():
            produce(j + FIRST)

    pl.semaphore_wait(far.at[2], AROUND)
    plane_neighbours(lambda device: pl.semaphore_signal(far.at[3], 1, device_id=device, device_id_type=MESH))

    sums = [jnp.sum(tacc[k], 0, keepdims=True) for k in range(5)]
    for p in range(NLINE):
        for k in range(5):
            tpc[p, k : k + 1, :] = sums[k][:, p * 128 : (p + 1) * 128]
    tr[line, 0:5, :] = tpc[line, 0:5, :]

    def line_copy(k, src, dst, i):
        return remote(src, dst, small_s.at[i], small_r.at[i], line_device(rem(line + k, NLINE)))

    @pl.loop(1, NLINE)
    def _(k):
        line_copy(k, tpc.at[rem(line + k, NLINE), pl.ds(0, 5)], tr.at[line, pl.ds(0, 5)], 0).start()

    def near_sums():
        drain(tr.at[pl.ds(0, NLINE - 1), pl.ds(0, 5)], small_r.at[0])
        tn[rem(zl, GROUP), 0:5, :] = jnp.sum(tr[:, 0:5, :], 0)

        def near_copy(k):
            mine = tn.at[rem(zl, GROUP), pl.ds(0, 5)]
            to = zl - rem(zl, GROUP) + rem(zl + k, GROUP)
            return remote(mine, mine, small_s.at[1], small_r.at[1], {"zl": to})

        @pl.loop(1, GROUP)
        def _(k):
            near_copy(k).start()

    def far_sums():
        drain(tn.at[pl.ds(0, GROUP - 1), pl.ds(0, 5)], small_r.at[1])
        tz[zl // GROUP, 0:5, :] = jnp.sum(tn[:, 0:5, :], 0)

        def far_copy(k):
            mine = tz.at[zl // GROUP, pl.ds(0, 5)]
            return remote(mine, mine, small_s.at[6], small_r.at[6], {"zl": rem(zl + k * GROUP, NZL)})

        @pl.loop(1, NZL // GROUP)
        def _(k):
            far_copy(k).start()

    pl.semaphore_wait(far.at[3], AROUND)

    @pl.loop(ahead, NCH)
    def _(j):
        forward(j)
        arrive(j - ahead)

    @pl.loop(NCH - ahead, NCH)
    def _(j):
        arrive(j)

    @pl.when(owner)
    def _():
        drain(gr.at[pl.ds(0, NPLANE - 1), pl.ds(0, PER)], small_r.at[2])
        za[z, 0:PER, :] = jnp.sum(gr[:, 0:PER, :], 0)

        def z_share(k):
            mine = za.at[z, pl.ds(0, PER)]
            remote(mine, mine, small_s.at[4], small_r.at[4], z_device(z + k)).start()

        z_share(NZ // 2)

        @pl.loop(1, NZ // 2)
        def _(k):
            z_share(NZ // 2 - k)
            z_share(NZ // 2 + k)

    average = jnp.sum(mean[...], -1, keepdims=True) * (1.0 / DIM)

    @pl.loop(0, NCH)
    def _(j):
        cols = pl.ds(pl.multiple_of(j * WIDE, WIDE), WIDE)
        value = (gain_of(j) * own[j] - xhat_of(j) * average) * inv[:, 0:1]
        out_o[:, cols] = value.astype(BF16)

    drain(tz.at[pl.ds(0, NZL // GROUP - 1), pl.ds(0, 5)], small_r.at[6])
    tf[line, 0:5, :] = jnp.sum(tz[:, 0:5, :], 0)

    @pl.loop(1, NLINE)
    def _(k):
        line_copy(k, tf.at[line, pl.ds(0, 5)], tf.at[line, pl.ds(0, 5)], 3).start()

    @pl.when(owner)
    def _():
        drain(za.at[pl.ds(0, NZ - 1), pl.ds(0, PER)], small_r.at[4])
        ga[place, 0:PER, :] = jnp.sum(za[:, 0:PER, :], 0)

        @pl.loop(0, NPLANE)
        def _(k):
            to = NPLANE - 1 - k

            @pl.when(to != place * NC + c)
            def _():
                mine = ga.at[place, pl.ds(0, PER)]
                remote(mine, mine, small_s.at[5], small_r.at[5], chip_at(to // NC, rem(to, NC))).start()

    drain(tf.at[pl.ds(0, NLINE - 1), pl.ds(0, 5)], small_r.at[3])
    for p in range(NLINE):
        taps_o[:, p * 128 : (p + 1) * 128] = tf[p, 0:4, :]
        bias_o[:, p * 128 : (p + 1) * 128] = tf[p, 4:5, :]

    @pl.when(has_next)
    def _():
        to_next.wait_send()

    @pl.when(has_prev)
    def _():
        for copy in to_prev:
            copy.wait_send()

    drain(ybuf.at[:, pl.ds(0, NY - 1)], ys_sem)
    drain(zs, zs_sem)
    drain(tr.at[pl.ds(0, NLINE - 1), pl.ds(0, 5)], small_s.at[0])
    drain(tn.at[pl.ds(0, GROUP - 1), pl.ds(0, 5)], small_s.at[1])
    drain(tz.at[pl.ds(0, NZL // GROUP - 1), pl.ds(0, 5)], small_s.at[6])
    drain(tf.at[pl.ds(0, NLINE - 1), pl.ds(0, 5)], small_s.at[3])

    @pl.when(owner)
    def _():
        drain(gr.at[pl.ds(0, NCH - 1), pl.ds(0, PER)], small_s.at[2])
        drain(za.at[pl.ds(0, NZ - 1), pl.ds(0, PER)], small_s.at[4])
        drain(ga.at[pl.ds(0, NCH - 1), pl.ds(0, PER)], small_r.at[5])

    @pl.when(jnp.logical_not(owner))
    def _():
        drain(gr.at[pl.ds(0, NCH), pl.ds(0, PER)], small_s.at[2])
        drain(ga.at[pl.ds(0, NCH), pl.ds(0, PER)], small_r.at[5])

    gain_o[...] = ga[:, 0:PER, :]

    @pl.when(owner)
    def _():
        drain(gr.at[pl.ds(0, NPLANE - 1), pl.ds(0, PER)], small_s.at[5])


def hand_on(*arrays):
    count = len(arrays)

    def body(*refs):
        sem = refs[2 * count]
        copies = [pltpu.make_async_copy(refs[i], refs[count + i], sem.at[i]) for i in range(count)]
        for copy in copies:
            copy.start()
        for copy in copies:
            copy.wait()

    return pl.pallas_call(
        body,
        out_shape=tuple(jax.ShapeDtypeStruct(a.shape, a.dtype) for a in arrays),
        in_specs=[pl.BlockSpec(memory_space=pltpu.VMEM)] * count,
        out_specs=(pl.BlockSpec(memory_space=pltpu.HBM),) * count,
        scratch_shapes=[pltpu.SemaphoreType.DMA((count,))],
        compiler_params=pltpu.CompilerParams(vmem_limit_bytes=4 << 20),
        name="hand_on",
    )(*arrays)


def on_device(hidden_in, norm_gain, proj_weight, conv_in, conv_weight, conv_bias, act_grad):
    vmem = pltpu.VMEM
    dma = pltpu.SemaphoreType.DMA
    out, gain, taps, bias = pl.pallas_call(
        kernel,
        out_shape=(
            jax.ShapeDtypeStruct((OWN, DIM), BF16),
            jax.ShapeDtypeStruct((NCH, PER, 128), F32),
            jax.ShapeDtypeStruct((4, CHAN), F32),
            jax.ShapeDtypeStruct((1, CHAN), F32),
        ),
        in_specs=[pl.BlockSpec(memory_space=pltpu.HBM)] * 7,
        out_specs=(pl.BlockSpec(memory_space=vmem),) * 4,
        scratch_shapes=[
            vmem((OWN, DIM), BF16),
            vmem((1, DIM), F32),
            vmem((DIM, CHAN), BF16),
            vmem((ROWS, CHAN), BF16),
            vmem((4, CHAN), F32),
            vmem((1, CHAN), F32),
            vmem((ROWS, CHAN), BF16),
            vmem((16, CHAN), BF16),
            vmem((16, CHAN), BF16),
            vmem((16, CHAN), BF16),
            vmem((ROWS + 16, CHAN), F32),
            vmem((ROWS + 8, CHAN), F32),
            vmem((ROWS, CHAN), BF16),
            vmem((5, 8, CHAN), F32),
            vmem((NCH, ROWS, WIDE), BF16),
            vmem((NCH, NY, PAIR, WIDE), BF16),
            vmem((NCH, OWN, WIDE), F32),
            vmem((NCH, OWN, WIDE), BF16),
            vmem((NCH, OWN, WIDE), BF16),
            vmem((OWN, 128), F32),
            vmem((OWN, 128), F32),
            vmem((NCH, 8, 128), F32),
            vmem((NPLANE, 8, 128), F32),
            vmem((NZ, 8, 128), F32),
            vmem((NCH, 8, 128), F32),
            vmem((NLINE, 8, 128), F32),
            vmem((NLINE, 8, 128), F32),
            vmem((GROUP, 8, 128), F32),
            vmem((NZL // GROUP, 8, 128), F32),
            vmem((NLINE, 8, 128), F32),
            dma((6,)),
            dma((WLOADS,)),
            dma((3,)),
            dma((3,)),
            dma,
            dma((NCH,)),
            dma,
            dma((NCH,)),
            dma((7,)),
            dma((7,)),
            pltpu.SemaphoreType.REGULAR((4,)),
        ],
        compiler_params=pltpu.CompilerParams(collective_id=0, has_side_effects=True, vmem_limit_bytes=40 << 20),
        name="layer_backward",
    )(
        *(
            pltpu.with_memory_space_constraint(a, pltpu.HBM)
            for a in (
                hidden_in,
                norm_gain.reshape(1, DIM),
                proj_weight,
                conv_in,
                conv_weight,
                conv_bias.reshape(1, CHAN),
                act_grad,
            )
        )
    )
    out, gain, taps, bias = hand_on(out, gain, taps, bias)
    return out, gain.reshape(DIM), taps, bias.reshape(CHAN)


def solution(mesh):
    finer = Mesh(mesh.devices.reshape(NZL, NX, NC, NY, NZH), ("zl", "x", "c", "y", "zh"))
    ctx = ("zl", "x", "c")
    tp = ("y", "zh")
    return jax.shard_map(
        on_device,
        mesh=finer,
        in_specs=(
            P(ctx + tp, None),
            P(),
            P(None, tp),
            P(ctx, tp),
            P(None, tp),
            P(tp),
            P(ctx, tp),
        ),
        out_specs=(P(ctx + tp, None), P(), P(None, tp), P(tp)),
        check_vma=False,
    )
```

```python
import jax
import jax.numpy as jnp
from jax import lax
from jax.experimental import pallas as pl
from jax.experimental.pallas import tpu as pltpu
from jax.sharding import Mesh
from jax.sharding import PartitionSpec as P

MESH = pl.DeviceIdType.MESH
NZL, NX, NC, NY, NZH = 16, 4, 2, 4, 2
NZ = NZL * NZH
NPLANE = NX * NC * NY
NLINE = NX * NC
NCTX = NZL * NX * NC
ROWS = 256
CHAN = 1024
DIM = 4096
NCH = 16
WIDE = DIM // NCH
PER = WIDE // 128
OWN = 32
PAIR = 64
TILE = 16
NEAR = 4
AROUND = NY - 1 + NX - 1 + NC - 1
WINDOW = 9
FIRST = 7
EXTRA = 3
WLOADS = 4
GROUP = 4
F32 = jnp.float32
CHIPS = sorted(
    ((i, j) for i in range(NX) for j in range(NY)), key=lambda p: -min(p[0], NX - p[0]) - min(p[1], NY - p[1])
)
CHIP_X = sum(p[0] << (2 * i) for i, p in enumerate(CHIPS))
CHIP_Y = sum(p[1] << (2 * i) for i, p in enumerate(CHIPS))
BF16 = jnp.bfloat16


def rem(a, b):
    return lax.rem(a, b)


def z_device(z):
    z = rem(z, NZ)
    return {"zh": z // NZL, "zl": rem(z, NZL)}


def plane_device(q):
    return {"x": q // (NY * NC), "y": rem(q // NC, NY), "c": rem(q, NC)}


def packed(table, i):
    signed = table - (1 << 32) if table >> 31 else table
    return lax.shift_right_logical(jnp.int32(signed), 2 * i) & 3


def chip_at(place, core):
    return {"x": packed(CHIP_X, place), "y": packed(CHIP_Y, place), "c": core}


def line_device(q):
    return {"x": q // NC, "c": rem(q, NC)}


def ctx_device(n):
    return {"zl": n // NLINE, "x": rem(n // NC, NX), "c": rem(n, NC)}


def kernel(
    hid_h, gain_h, w_h, conv_h, cw_h, cb_h, act_h,
    out_o, gain_o, taps_o, bias_o,
    hid, gain, w, conv, cw, cb, act,
    hprev, hconv, hact,
    xf, pg, ing, tacc,
    pbuf, ybuf, own, zs, zr, inv, mean,
    gbuf, gr, za, ga, tpc, tr, tn, tz, tf,
    in_sem, w_sem, hs_sem, hr_sem, ys_sem, yr_sem, zs_sem, zr_sem, small_s, small_r, far,
):
    zl = lax.axis_index("zl")
    zh = lax.axis_index("zh")
    x = lax.axis_index("x")
    y = lax.axis_index("y")
    c = lax.axis_index("c")
    z = zh * NZL + zl
    q = (x * NY + y) * NC + c
    line = x * NC + c
    place = sum(jnp.where(jnp.logical_and(x == a, y == b), i, 0) for i, (a, b) in enumerate(CHIPS))
    owner = c == NC - 1
    ahead = WINDOW + EXTRA * (1 - c)
    n = zl * NLINE + line
    has_next = n < NCTX - 1
    has_prev = n > 0
    chip_next = jnp.logical_and(c == NC - 1, has_next)
    chip_prev = jnp.logical_and(c == 0, has_prev)

    def remote(src, dst, send, recv, device):
        return pltpu.make_async_remote_copy(
            src_ref=src, dst_ref=dst, send_sem=send, recv_sem=recv, device_id=device, device_id_type=MESH
        )

    def drain(ref, sem):
        pltpu.make_async_copy(ref, ref, sem).wait()

    loads = [
        pltpu.make_async_copy(a, b, in_sem.at[i])
        for i, (a, b) in enumerate(
            [
                (conv_h, conv),
                (act_h, act),
                (cw_h, cw),
                (cb_h, cb),
                (hid_h, hid),
                (gain_h, gain),
            ]
        )
    ]
    for load in loads[:4]:
        load.start()

    barrier = pltpu.get_barrier_semaphore()

    def greet(device):
        pl.semaphore_signal(barrier, 1, device_id=device, device_id_type=MESH)

    def plane_neighbours(visit):
        for k in (2, 1, 3):
            visit({"y": rem(y + k, NY)})
            visit({"x": rem(x + k, NX)})
        visit({"c": 1 - c})

    @pl.loop(0, NEAR)
    def _(k):
        greet(z_device(z + (NEAR - k)))
        greet(z_device(z + NZ - (NEAR - k)))

    plane_neighbours(greet)

    @pl.when(chip_next)
    def _():
        greet(ctx_device(n + 1))

    @pl.when(chip_prev)
    def _():
        greet(ctx_device(n - 1))

    for load in loads[4:]:
        load.start()

    def w_load(i):
        rows = pl.ds(pl.multiple_of(i * (DIM // WLOADS), DIM // WLOADS), DIM // WLOADS)
        return pltpu.make_async_copy(w_h.at[rows], w.at[rows], w_sem.at[i])

    @pl.loop(0, WLOADS)
    def _(i):
        w_load(i).start()

    xf[0:8, :] = jnp.zeros((8, CHAN), F32)
    tacc[...] = jnp.zeros_like(tacc)
    loads[0].wait()

    @pl.loop(0, ROWS // TILE)
    def _(i):
        t = pl.multiple_of(i * TILE, TILE)
        xf[pl.ds(t + 8, TILE), :] = conv[pl.ds(t, TILE), :].astype(F32)

    for load in loads[1:4]:
        load.wait()

    def grad_tile(t, rows, cotangent):
        above = xf[pl.ds(t, rows + 8), :]
        xs = [above[8 - k : 8 - k + rows] for k in range(4)]
        pre = cb[0:1, :] + sum(cw[k : k + 1, :] * xs[k] for k in range(4))
        s = 1.0 / (1.0 + jnp.exp(-pre))
        return cotangent * s * (1.0 + pre * (1.0 - s)), xs

    def pass_one(i):
        t = pl.multiple_of(i * TILE, TILE)
        g, xs = grad_tile(t, TILE, act[pl.ds(t, TILE), :].astype(F32))
        pg[pl.ds(t, TILE), :] = g
        for k in range(5):
            term = g * xs[k] if k < 4 else g
            tacc[k] += term[0:8] + term[8:16]

    def pass_two(i):
        t = pl.multiple_of(i * TILE, TILE)
        below = pg[pl.ds(t, TILE + 8), :]
        total = sum(cw[k : k + 1, :] * below[k : k + TILE] for k in range(4))
        ing[pl.ds(t, TILE), :] = total.astype(BF16)

    last = ROWS // TILE - 1

    @pl.loop(1, last + 1)
    def _(i):
        pass_one(i)

    pl.semaphore_wait(
        barrier,
        AROUND + 2 * NEAR + jnp.where(chip_next, 1, 0) + jnp.where(chip_prev, 1, 0),
    )
    for step in (NEAR, NZ - NEAR):
        pl.semaphore_signal(far.at[0], 1, device_id=z_device(z + step), device_id_type=MESH)

    to_next = remote(conv.at[pl.ds(ROWS - 16, 16)], hprev, hs_sem.at[0], hr_sem.at[0], ctx_device(jnp.minimum(n + 1, NCTX - 1)))
    to_prev = [
        remote(conv.at[pl.ds(0, 16)], hconv, hs_sem.at[1], hr_sem.at[1], ctx_device(jnp.maximum(n - 1, 0))),
        remote(act.at[pl.ds(0, 16)], hact, hs_sem.at[2], hr_sem.at[2], ctx_device(jnp.maximum(n - 1, 0))),
    ]

    @pl.when(has_next)
    def _():
        to_next.start()

    @pl.when(has_prev)
    def _():
        for copy in to_prev:
            copy.start()

    plane_neighbours(lambda device: pl.semaphore_signal(far.at[2], 1, device_id=device, device_id_type=MESH))

    @pl.loop(1, last)
    def _(i):
        pass_two(i)

    loads[4].wait()
    loads[5].wait()

    def squares(j, total):
        cols = pl.ds(pl.multiple_of(j * WIDE, WIDE), WIDE)
        h = hid[:, cols].astype(F32)
        h = h * h
        return total + sum(h[:, i * 128 : (i + 1) * 128] for i in range(PER))

    square = lax.fori_loop(0, NCH, squares, jnp.zeros((OWN, 128), F32))
    rms = jnp.sqrt(jnp.sum(square, -1, keepdims=True) * (1.0 / DIM) + 1e-05)
    inv[...] = jnp.broadcast_to(1.0 / rms, (OWN, 128))
    pl.semaphore_wait(far.at[0], 2)
    for step in (2 * NEAR, NZ - 2 * NEAR):
        pl.semaphore_signal(far.at[1], 1, device_id=z_device(z + step), device_id_type=MESH)

    @pl.when(has_prev)
    def _():
        to_next.wait_recv()
        xf[0:8, :] = hprev[8:16, :].astype(F32)

    pass_one(0)
    pass_two(0)

    @pl.when(has_next)
    def _():
        for copy in to_prev:
            copy.wait_recv()
        xf[ROWS + 8 : ROWS + 16, :] = hconv[0:8, :].astype(F32)
        g, _ = grad_tile(ROWS, 8, hact[0:8, :].astype(F32))
        pg[ROWS : ROWS + 8, :] = g

    @pl.when(jnp.logical_not(has_next))
    def _():
        pg[ROWS : ROWS + 8, :] = jnp.zeros((8, CHAN), F32)

    pass_two(last)

    def product(j):
        rows = pl.ds(pl.multiple_of(j * WIDE, WIDE), WIDE)

        @pl.when(rem(j, NCH // WLOADS) == 0)
        def _():
            w_load(j // (NCH // WLOADS)).wait()

        part = lax.dot_general(ing[...], w[rows, :], (((1,), (1,)), ((), ())), preferred_element_type=F32)
        pbuf[j] = part.astype(BF16)

    def y_copy(j, k):
        to = rem(y + k, NY)
        return remote(
            pbuf.at[j, pl.ds(pl.multiple_of(to * PAIR, PAIR), PAIR)],
            ybuf.at[j, y],
            ys_sem,
            yr_sem.at[j],
            {"y": to},
        )

    def y_send(j):
        for k in range(1, NY):
            y_copy(j, k).start()

    def produce(j):
        product(j)
        y_send(j - 1)

        @pl.when(j == NCH - 1)
        def _():
            y_send(j)

    product(0)

    @pl.loop(1, FIRST)
    def _(j):
        produce(j)


    def z_copy(j):
        return remote(zs.at[j], zr.at[j], zs_sem, zr_sem.at[j], {"zh": 1 - zh})

    mine = pl.multiple_of(zh * OWN, OWN)
    other = pl.multiple_of((1 - zh) * OWN, OWN)

    def xhat_of(j):
        cols = pl.ds(pl.multiple_of(j * WIDE, WIDE), WIDE)
        return hid[:, cols].astype(F32) * inv[:, 0:1]

    def gain_of(j):
        return gain[0:1, pl.ds(pl.multiple_of(j * WIDE, WIDE), WIDE)]

    def share(j, sums):
        for i in range(PER):
            gbuf[j, i : i + 1, :] = sums[:, i * 128 : (i + 1) * 128]

    def share_send(j):
        mine = jnp.logical_and(j == place, owner)

        @pl.when(jnp.logical_not(mine))
        def _():
            remote(
                gbuf.at[j, pl.ds(0, PER)],
                gr.at[q, pl.ds(0, PER)],
                small_s.at[2],
                small_r.at[2],
                chip_at(j, NC - 1),
            ).start()

        @pl.when(mine)
        def _():
            gr[q, 0:PER, :] = gbuf[j, 0:PER, :]

    def arrive(j):
        z_copy(j).wait_recv()
        normed = own[j] + zr[j].astype(F32)
        own[j] = normed
        both = normed * xhat_of(j)
        share(j, jnp.sum(both, 0, keepdims=True))
        both = both * gain_of(j)
        mean[...] += sum(both[:, i * 128 : (i + 1) * 128] for i in range(PER))
        share_send(j)

        @pl.when(j == 3)
        def _():
            near_sums()

        @pl.when(j == 10)
        def _():
            far_sums()

    def forward(j):
        drain(ybuf.at[j, pl.ds(0, NY - 1)], yr_sem.at[j])
        ybuf[j, y] = pbuf[j, pl.ds(pl.multiple_of(y * PAIR, PAIR), PAIR), :]

        def total(start):
            return sum(ybuf[j, s, pl.ds(start, OWN), :].astype(F32) for s in range(NY))

        zs[j] = total(other).astype(BF16)
        own[j] = total(mine)
        z_copy(j).start()

    mean[...] = jnp.zeros_like(mean)
    pl.semaphore_wait(far.at[1], 2)

    @pl.loop(0, ahead)
    def _(j):
        forward(j)

        @pl.when(j + FIRST < NCH)
        def _():
            produce(j + FIRST)

    pl.semaphore_wait(far.at[2], AROUND)
    plane_neighbours(lambda device: pl.semaphore_signal(far.at[3], 1, device_id=device, device_id_type=MESH))

    sums = [jnp.sum(tacc[k], 0, keepdims=True) for k in range(5)]
    for p in range(NLINE):
        for k in range(5):
            tpc[p, k : k + 1, :] = sums[k][:, p * 128 : (p + 1) * 128]
    tr[line, 0:5, :] = tpc[line, 0:5, :]

    def line_copy(k, src, dst, i):
        return remote(src, dst, small_s.at[i], small_r.at[i], line_device(rem(line + k, NLINE)))

    @pl.loop(1, NLINE)
    def _(k):
        line_copy(k, tpc.at[rem(line + k, NLINE), pl.ds(0, 5)], tr.at[line, pl.ds(0, 5)], 0).start()

    def near_sums():
        drain(tr.at[pl.ds(0, NLINE - 1), pl.ds(0, 5)], small_r.at[0])
        tn[rem(zl, GROUP), 0:5, :] = jnp.sum(tr[:, 0:5, :], 0)

        def near_copy(k):
            mine = tn.at[rem(zl, GROUP), pl.ds(0, 5)]
            to = zl - rem(zl, GROUP) + rem(zl + k, GROUP)
            return remote(mine, mine, small_s.at[1], small_r.at[1], {"zl": to})

        @pl.loop(1, GROUP)
        def _(k):
            near_copy(k).start()

    def far_sums():
        drain(tn.at[pl.ds(0, GROUP - 1), pl.ds(0, 5)], small_r.at[1])
        tz[zl // GROUP, 0:5, :] = jnp.sum(tn[:, 0:5, :], 0)

        def far_copy(k):
            mine = tz.at[zl // GROUP, pl.ds(0, 5)]
            return remote(mine, mine, small_s.at[6], small_r.at[6], {"zl": rem(zl + k * GROUP, NZL)})

        @pl.loop(1, NZL // GROUP)
        def _(k):
            far_copy(k).start()

    pl.semaphore_wait(far.at[3], AROUND)

    @pl.loop(ahead, NCH)
    def _(j):
        forward(j)
        arrive(j - ahead)

    @pl.loop(NCH - ahead, NCH)
    def _(j):
        arrive(j)

    @pl.when(owner)
    def _():
        drain(gr.at[pl.ds(0, NPLANE - 1), pl.ds(0, PER)], small_r.at[2])
        za[z, 0:PER, :] = jnp.sum(gr[:, 0:PER, :], 0)

        def z_share(k):
            mine = za.at[z, pl.ds(0, PER)]
            remote(mine, mine, small_s.at[4], small_r.at[4], z_device(z + k)).start()

        z_share(NZ // 2)

        for k in range(1, NZ // 2):
            z_share(NZ // 2 - k)
            z_share(NZ // 2 + k)

    average = jnp.sum(mean[...], -1, keepdims=True) * (1.0 / DIM)

    @pl.loop(0, NCH)
    def _(j):
        cols = pl.ds(pl.multiple_of(j * WIDE, WIDE), WIDE)
        value = (gain_of(j) * own[j] - xhat_of(j) * average) * inv[:, 0:1]
        out_o[:, cols] = value.astype(BF16)

    drain(tz.at[pl.ds(0, NZL // GROUP - 1), pl.ds(0, 5)], small_r.at[6])
    tf[line, 0:5, :] = jnp.sum(tz[:, 0:5, :], 0)

    @pl.loop(1, NLINE)
    def _(k):
        line_copy(k, tf.at[line, pl.ds(0, 5)], tf.at[line, pl.ds(0, 5)], 3).start()

    drain(tf.at[pl.ds(0, NLINE - 1), pl.ds(0, 5)], small_r.at[3])
    for p in range(NLINE):
        taps_o[:, p * 128 : (p + 1) * 128] = tf[p, 0:4, :]
        bias_o[:, p * 128 : (p + 1) * 128] = tf[p, 4:5, :]

    @pl.when(has_next)
    def _():
        to_next.wait_send()

    @pl.when(has_prev)
    def _():
        for copy in to_prev:
            copy.wait_send()

    drain(ybuf.at[:, pl.ds(0, NY - 1)], ys_sem)
    drain(zs, zs_sem)
    drain(tr.at[pl.ds(0, NLINE - 1), pl.ds(0, 5)], small_s.at[0])
    drain(tn.at[pl.ds(0, GROUP - 1), pl.ds(0, 5)], small_s.at[1])
    drain(tz.at[pl.ds(0, NZL // GROUP - 1), pl.ds(0, 5)], small_s.at[6])
    drain(tf.at[pl.ds(0, NLINE - 1), pl.ds(0, 5)], small_s.at[3])

    @pl.when(owner)
    def _():
        drain(gr.at[pl.ds(0, NCH - 1), pl.ds(0, PER)], small_s.at[2])
        drain(za.at[pl.ds(0, NZ - 1), pl.ds(0, PER)], small_s.at[4])

    @pl.when(jnp.logical_not(owner))
    def _():
        drain(gr.at[pl.ds(0, NCH), pl.ds(0, PER)], small_s.at[2])

    @pl.when(owner)
    def _():
        drain(za.at[pl.ds(0, NZ - 1), pl.ds(0, PER)], small_r.at[4])
        ga[place, 0:PER, :] = jnp.sum(za[:, 0:PER, :], 0)

        mine = ga.at[place, pl.ds(0, PER)]
        for i, j in reversed(CHIPS):
            for core in reversed(range(NC)):
                here = (x == i) & (y == j) & (c == core)

                @pl.when(jnp.logical_not(here))
                def _():
                    to = {"x": i, "y": j, "c": core}
                    remote(mine, mine, small_s.at[5], small_r.at[5], to).start()

    @pl.when(owner)
    def _():
        drain(ga.at[pl.ds(0, NCH - 1), pl.ds(0, PER)], small_r.at[5])

    @pl.when(jnp.logical_not(owner))
    def _():
        drain(ga.at[pl.ds(0, NCH), pl.ds(0, PER)], small_r.at[5])

    gain_o[...] = ga[:, 0:PER, :]

    @pl.when(owner)
    def _():
        drain(gr.at[pl.ds(0, NPLANE - 1), pl.ds(0, PER)], small_s.at[5])


def hand_on(*arrays):
    count = len(arrays)

    def body(*refs):
        sem = refs[2 * count]
        copies = [pltpu.make_async_copy(refs[i], refs[count + i], sem.at[i]) for i in range(count)]
        for copy in copies:
            copy.start()
        for copy in copies:
            copy.wait()

    return pl.pallas_call(
        body,
        out_shape=tuple(jax.ShapeDtypeStruct(a.shape, a.dtype) for a in arrays),
        in_specs=[pl.BlockSpec(memory_space=pltpu.VMEM)] * count,
        out_specs=(pl.BlockSpec(memory_space=pltpu.HBM),) * count,
        scratch_shapes=[pltpu.SemaphoreType.DMA((count,))],
        compiler_params=pltpu.CompilerParams(vmem_limit_bytes=4 << 20),
        name="hand_on",
    )(*arrays)


def on_device(hidden_in, norm_gain, proj_weight, conv_in, conv_weight, conv_bias, act_grad):
    vmem = pltpu.VMEM
    dma = pltpu.SemaphoreType.DMA
    out, gain, taps, bias = pl.pallas_call(
        kernel,
        out_shape=(
            jax.ShapeDtypeStruct((OWN, DIM), BF16),
            jax.ShapeDtypeStruct((NCH, PER, 128), F32),
            jax.ShapeDtypeStruct((4, CHAN), F32),
            jax.ShapeDtypeStruct((1, CHAN), F32),
        ),
        in_specs=[pl.BlockSpec(memory_space=pltpu.HBM)] * 7,
        out_specs=(pl.BlockSpec(memory_space=vmem),) * 4,
        scratch_shapes=[
            vmem((OWN, DIM), BF16),
            vmem((1, DIM), F32),
            vmem((DIM, CHAN), BF16),
            vmem((ROWS, CHAN), BF16),
            vmem((4, CHAN), F32),
            vmem((1, CHAN), F32),
            vmem((ROWS, CHAN), BF16),
            vmem((16, CHAN), BF16),
            vmem((16, CHAN), BF16),
            vmem((16, CHAN), BF16),
            vmem((ROWS + 16, CHAN), F32),
            vmem((ROWS + 8, CHAN), F32),
            vmem((ROWS, CHAN), BF16),
            vmem((5, 8, CHAN), F32),
            vmem((NCH, ROWS, WIDE), BF16),
            vmem((NCH, NY, PAIR, WIDE), BF16),
            vmem((NCH, OWN, WIDE), F32),
            vmem((NCH, OWN, WIDE), BF16),
            vmem((NCH, OWN, WIDE), BF16),
            vmem((OWN, 128), F32),
            vmem((OWN, 128), F32),
            vmem((NCH, 8, 128), F32),
            vmem((NPLANE, 8, 128), F32),
            vmem((NZ, 8, 128), F32),
            vmem((NCH, 8, 128), F32),
            vmem((NLINE, 8, 128), F32),
            vmem((NLINE, 8, 128), F32),
            vmem((GROUP, 8, 128), F32),
            vmem((NZL // GROUP, 8, 128), F32),
            vmem((NLINE, 8, 128), F32),
            dma((6,)),
            dma((WLOADS,)),
            dma((3,)),
            dma((3,)),
            dma,
            dma((NCH,)),
            dma,
            dma((NCH,)),
            dma((7,)),
            dma((7,)),
            pltpu.SemaphoreType.REGULAR((4,)),
        ],
        compiler_params=pltpu.CompilerParams(collective_id=0, has_side_effects=True, vmem_limit_bytes=40 << 20),
        name="layer_backward",
    )(
        *(
            pltpu.with_memory_space_constraint(a, pltpu.HBM)
            for a in (
                hidden_in,
                norm_gain.reshape(1, DIM),
                proj_weight,
                conv_in,
                conv_weight,
                conv_bias.reshape(1, CHAN),
                act_grad,
            )
        )
    )
    out, gain, taps, bias = hand_on(out, gain, taps, bias)
    return out, gain.reshape(DIM), taps, bias.reshape(CHAN)


def solution(mesh):
    finer = Mesh(mesh.devices.reshape(NZL, NX, NC, NY, NZH), ("zl", "x", "c", "y", "zh"))
    ctx = ("zl", "x", "c")
    tp = ("y", "zh")
    return jax.shard_map(
        on_device,
        mesh=finer,
        in_specs=(
            P(ctx + tp, None),
            P(),
            P(None, tp),
            P(ctx, tp),
            P(None, tp),
            P(tp),
            P(ctx, tp),
        ),
        out_specs=(P(ctx + tp, None), P(), P(None, tp), P(tp)),
        check_vma=False,
    )
```

```python
import jax
import jax.numpy as jnp
from jax import lax
from jax.experimental import pallas as pl
from jax.experimental.pallas import tpu as pltpu
from jax.sharding import Mesh
from jax.sharding import PartitionSpec as P

MESH = pl.DeviceIdType.MESH
NZL, NX, NC, NY, NZH = 16, 4, 2, 4, 2
NZ = NZL * NZH
NPLANE = NX * NC * NY
NLINE = NX * NC
NCTX = NZL * NX * NC
ROWS = 256
CHAN = 1024
DIM = 4096
NCH = 16
WIDE = DIM // NCH
PER = WIDE // 128
OWN = 32
PAIR = 64
TILE = 16
NEAR = 4
AROUND = NY - 1 + NX - 1 + NC - 1
WINDOW = 9
FIRST = 7
EXTRA = 3
WLOADS = 4
GROUP = 4
F32 = jnp.float32
CHIPS = sorted(
    ((i, j) for i in range(NX) for j in range(NY)), key=lambda p: -min(p[0], NX - p[0]) - min(p[1], NY - p[1])
)
CHIP_X = sum(p[0] << (2 * i) for i, p in enumerate(CHIPS))
CHIP_Y = sum(p[1] << (2 * i) for i, p in enumerate(CHIPS))
BF16 = jnp.bfloat16


def rem(a, b):
    return lax.rem(a, b)


def z_device(z):
    z = rem(z, NZ)
    return {"zh": z // NZL, "zl": rem(z, NZL)}


def plane_device(q):
    return {"x": q // (NY * NC), "y": rem(q // NC, NY), "c": rem(q, NC)}


def packed(table, i):
    signed = table - (1 << 32) if table >> 31 else table
    return lax.shift_right_logical(jnp.int32(signed), 2 * i) & 3


def chip_at(place, core):
    return {"x": packed(CHIP_X, place), "y": packed(CHIP_Y, place), "c": core}


def line_device(q):
    return {"x": q // NC, "c": rem(q, NC)}


def ctx_device(n):
    return {"zl": n // NLINE, "x": rem(n // NC, NX), "c": rem(n, NC)}


def kernel(
    hid_h, gain_h, w_h, conv_h, cw_h, cb_h, act_h,
    out_o, gain_o, taps_o, bias_o,
    hid, gain, w, conv, cw, cb, act,
    hprev, hconv, hact,
    xf, pg, ing, tacc,
    pbuf, ybuf, own, zs, zr, inv, mean,
    gbuf, gr, za, ga, tpc, tr, tn, tz, tf,
    in_sem, w_sem, hs_sem, hr_sem, ys_sem, yr_sem, zs_sem, zr_sem, small_s, small_r, far,
):
    zl = lax.axis_index("zl")
    zh = lax.axis_index("zh")
    x = lax.axis_index("x")
    y = lax.axis_index("y")
    c = lax.axis_index("c")
    z = zh * NZL + zl
    q = (x * NY + y) * NC + c
    line = x * NC + c
    place = sum(jnp.where(jnp.logical_and(x == a, y == b), i, 0) for i, (a, b) in enumerate(CHIPS))
    owner = c == NC - 1
    ahead = WINDOW + EXTRA * (1 - c)
    n = zl * NLINE + line
    has_next = n < NCTX - 1
    has_prev = n > 0
    chip_next = jnp.logical_and(c == NC - 1, has_next)
    chip_prev = jnp.logical_and(c == 0, has_prev)

    def remote(src, dst, send, recv, device):
        return pltpu.make_async_remote_copy(
            src_ref=src, dst_ref=dst, send_sem=send, recv_sem=recv, device_id=device, device_id_type=MESH
        )

    def drain(ref, sem):
        pltpu.make_async_copy(ref, ref, sem).wait()

    loads = [
        pltpu.make_async_copy(a, b, in_sem.at[i])
        for i, (a, b) in enumerate(
            [
                (conv_h, conv),
                (act_h, act),
                (cw_h, cw),
                (cb_h, cb),
                (hid_h, hid),
                (gain_h, gain),
            ]
        )
    ]
    for load in loads[:4]:
        load.start()

    barrier = pltpu.get_barrier_semaphore()

    def greet(device):
        pl.semaphore_signal(barrier, 1, device_id=device, device_id_type=MESH)

    def plane_neighbours(visit):
        for k in (2, 1, 3):
            visit({"y": rem(y + k, NY)})
            visit({"x": rem(x + k, NX)})
        visit({"c": 1 - c})

    @pl.loop(0, NEAR)
    def _(k):
        greet(z_device(z + (NEAR - k)))
        greet(z_device(z + NZ - (NEAR - k)))

    plane_neighbours(greet)

    @pl.when(chip_next)
    def _():
        greet(ctx_device(n + 1))

    @pl.when(chip_prev)
    def _():
        greet(ctx_device(n - 1))

    for load in loads[4:]:
        load.start()

    def w_load(i):
        rows = pl.ds(pl.multiple_of(i * (DIM // WLOADS), DIM // WLOADS), DIM // WLOADS)
        return pltpu.make_async_copy(w_h.at[rows], w.at[rows], w_sem.at[i])

    @pl.loop(0, WLOADS)
    def _(i):
        w_load(i).start()

    xf[0:8, :] = jnp.zeros((8, CHAN), F32)
    tacc[...] = jnp.zeros_like(tacc)
    loads[0].wait()

    @pl.loop(0, ROWS // TILE)
    def _(i):
        t = pl.multiple_of(i * TILE, TILE)
        xf[pl.ds(t + 8, TILE), :] = conv[pl.ds(t, TILE), :].astype(F32)

    for load in loads[1:4]:
        load.wait()

    def grad_tile(t, rows, cotangent):
        above = xf[pl.ds(t, rows + 8), :]
        xs = [above[8 - k : 8 - k + rows] for k in range(4)]
        pre = cb[0:1, :] + sum(cw[k : k + 1, :] * xs[k] for k in range(4))
        s = 1.0 / (1.0 + jnp.exp(-pre))
        return cotangent * s * (1.0 + pre * (1.0 - s)), xs

    def pass_one(i):
        t = pl.multiple_of(i * TILE, TILE)
        g, xs = grad_tile(t, TILE, act[pl.ds(t, TILE), :].astype(F32))
        pg[pl.ds(t, TILE), :] = g
        for k in range(5):
            term = g * xs[k] if k < 4 else g
            tacc[k] += term[0:8] + term[8:16]

    def pass_two(i):
        t = pl.multiple_of(i * TILE, TILE)
        below = pg[pl.ds(t, TILE + 8), :]
        total = sum(cw[k : k + 1, :] * below[k : k + TILE] for k in range(4))
        ing[pl.ds(t, TILE), :] = total.astype(BF16)

    last = ROWS // TILE - 1

    @pl.loop(1, last + 1)
    def _(i):
        pass_one(i)

    pl.semaphore_wait(
        barrier,
        AROUND + 2 * NEAR + jnp.where(chip_next, 1, 0) + jnp.where(chip_prev, 1, 0),
    )
    for step in (NEAR, NZ - NEAR):
        pl.semaphore_signal(far.at[0], 1, device_id=z_device(z + step), device_id_type=MESH)

    to_next = remote(conv.at[pl.ds(ROWS - 16, 16)], hprev, hs_sem.at[0], hr_sem.at[0], ctx_device(jnp.minimum(n + 1, NCTX - 1)))
    to_prev = [
        remote(conv.at[pl.ds(0, 16)], hconv, hs_sem.at[1], hr_sem.at[1], ctx_device(jnp.maximum(n - 1, 0))),
        remote(act.at[pl.ds(0, 16)], hact, hs_sem.at[2], hr_sem.at[2], ctx_device(jnp.maximum(n - 1, 0))),
    ]

    @pl.when(has_next)
    def _():
        to_next.start()

    @pl.when(has_prev)
    def _():
        for copy in to_prev:
            copy.start()

    plane_neighbours(lambda device: pl.semaphore_signal(far.at[2], 1, device_id=device, device_id_type=MESH))

    @pl.loop(1, last)
    def _(i):
        pass_two(i)

    loads[4].wait()
    loads[5].wait()

    def squares(j, total):
        cols = pl.ds(pl.multiple_of(j * WIDE, WIDE), WIDE)
        h = hid[:, cols].astype(F32)
        h = h * h
        return total + sum(h[:, i * 128 : (i + 1) * 128] for i in range(PER))

    square = lax.fori_loop(0, NCH, squares, jnp.zeros((OWN, 128), F32))
    rms = jnp.sqrt(jnp.sum(square, -1, keepdims=True) * (1.0 / DIM) + 1e-05)
    inv[...] = jnp.broadcast_to(1.0 / rms, (OWN, 128))
    pl.semaphore_wait(far.at[0], 2)
    for step in (2 * NEAR, NZ - 2 * NEAR):
        pl.semaphore_signal(far.at[1], 1, device_id=z_device(z + step), device_id_type=MESH)

    @pl.when(has_prev)
    def _():
        to_next.wait_recv()
        xf[0:8, :] = hprev[8:16, :].astype(F32)

    pass_one(0)
    pass_two(0)

    @pl.when(has_next)
    def _():
        for copy in to_prev:
            copy.wait_recv()
        xf[ROWS + 8 : ROWS + 16, :] = hconv[0:8, :].astype(F32)
        g, _ = grad_tile(ROWS, 8, hact[0:8, :].astype(F32))
        pg[ROWS : ROWS + 8, :] = g

    @pl.when(jnp.logical_not(has_next))
    def _():
        pg[ROWS : ROWS + 8, :] = jnp.zeros((8, CHAN), F32)

    pass_two(last)

    def product(j):
        rows = pl.ds(pl.multiple_of(j * WIDE, WIDE), WIDE)

        @pl.when(rem(j, NCH // WLOADS) == 0)
        def _():
            w_load(j // (NCH // WLOADS)).wait()

        part = lax.dot_general(ing[...], w[rows, :], (((1,), (1,)), ((), ())), preferred_element_type=F32)
        pbuf[j] = part.astype(BF16)

    def y_copy(j, k):
        to = rem(y + k, NY)
        return remote(
            pbuf.at[j, pl.ds(pl.multiple_of(to * PAIR, PAIR), PAIR)],
            ybuf.at[j, y],
            ys_sem,
            yr_sem.at[j],
            {"y": to},
        )

    def y_send(j):
        for k in range(1, NY):
            y_copy(j, k).start()

    def produce(j):
        product(j)
        y_send(j - 1)

        @pl.when(j == NCH - 1)
        def _():
            y_send(j)

    product(0)

    @pl.loop(1, FIRST)
    def _(j):
        produce(j)


    def z_copy(j):
        return remote(zs.at[j], zr.at[j], zs_sem, zr_sem.at[j], {"zh": 1 - zh})

    mine = pl.multiple_of(zh * OWN, OWN)
    other = pl.multiple_of((1 - zh) * OWN, OWN)

    def xhat_of(j):
        cols = pl.ds(pl.multiple_of(j * WIDE, WIDE), WIDE)
        return hid[:, cols].astype(F32) * inv[:, 0:1]

    def gain_of(j):
        return gain[0:1, pl.ds(pl.multiple_of(j * WIDE, WIDE), WIDE)]

    def share(j, sums):
        for i in range(PER):
            gbuf[j, i : i + 1, :] = sums[:, i * 128 : (i + 1) * 128]

    def share_send(j):
        mine = jnp.logical_and(j == place, owner)

        @pl.when(jnp.logical_not(mine))
        def _():
            remote(
                gbuf.at[j, pl.ds(0, PER)],
                gr.at[q, pl.ds(0, PER)],
                small_s.at[2],
                small_r.at[2],
                chip_at(j, NC - 1),
            ).start()

        @pl.when(mine)
        def _():
            gr[q, 0:PER, :] = gbuf[j, 0:PER, :]

    def arrive(j):
        z_copy(j).wait_recv()
        normed = own[j] + zr[j].astype(F32)
        own[j] = normed
        both = normed * xhat_of(j)
        share(j, jnp.sum(both, 0, keepdims=True))
        both = both * gain_of(j)
        mean[...] += sum(both[:, i * 128 : (i + 1) * 128] for i in range(PER))
        share_send(j)

        @pl.when(j == 3)
        def _():
            near_sums()

        @pl.when(j == 10)
        def _():
            far_sums()

    def forward(j):
        drain(ybuf.at[j, pl.ds(0, NY - 1)], yr_sem.at[j])
        ybuf[j, y] = pbuf[j, pl.ds(pl.multiple_of(y * PAIR, PAIR), PAIR), :]

        def total(start):
            return sum(ybuf[j, s, pl.ds(start, OWN), :].astype(F32) for s in range(NY))

        zs[j] = total(other).astype(BF16)
        own[j] = total(mine)
        z_copy(j).start()

    pl.semaphore_wait(far.at[2], AROUND)
    plane_neighbours(lambda device: pl.semaphore_signal(far.at[3], 1, device_id=device, device_id_type=MESH))

    mean[...] = jnp.zeros_like(mean)
    pl.semaphore_wait(far.at[1], 2)

    @pl.loop(0, ahead)
    def _(j):
        forward(j)

        @pl.when(j + FIRST < NCH)
        def _():
            produce(j + FIRST)


    sums = [jnp.sum(tacc[k], 0, keepdims=True) for k in range(5)]
    for p in range(NLINE):
        for k in range(5):
            tpc[p, k : k + 1, :] = sums[k][:, p * 128 : (p + 1) * 128]
    tr[line, 0:5, :] = tpc[line, 0:5, :]

    def line_copy(k, src, dst, i):
        return remote(src, dst, small_s.at[i], small_r.at[i], line_device(rem(line + k, NLINE)))

    @pl.loop(1, NLINE)
    def _(k):
        line_copy(k, tpc.at[rem(line + k, NLINE), pl.ds(0, 5)], tr.at[line, pl.ds(0, 5)], 0).start()

    def near_sums():
        drain(tr.at[pl.ds(0, NLINE - 1), pl.ds(0, 5)], small_r.at[0])
        tn[rem(zl, GROUP), 0:5, :] = jnp.sum(tr[:, 0:5, :], 0)

        def near_copy(k):
            mine = tn.at[rem(zl, GROUP), pl.ds(0, 5)]
            to = zl - rem(zl, GROUP) + rem(zl + k, GROUP)
            return remote(mine, mine, small_s.at[1], small_r.at[1], {"zl": to})

        @pl.loop(1, GROUP)
        def _(k):
            near_copy(k).start()

    def far_sums():
        drain(tn.at[pl.ds(0, GROUP - 1), pl.ds(0, 5)], small_r.at[1])
        tz[zl // GROUP, 0:5, :] = jnp.sum(tn[:, 0:5, :], 0)

        def far_copy(k):
            mine = tz.at[zl // GROUP, pl.ds(0, 5)]
            return remote(mine, mine, small_s.at[6], small_r.at[6], {"zl": rem(zl + k * GROUP, NZL)})

        @pl.loop(1, NZL // GROUP)
        def _(k):
            far_copy(k).start()

    pl.semaphore_wait(far.at[3], AROUND)

    @pl.loop(ahead, NCH)
    def _(j):
        forward(j)
        arrive(j - ahead)

    @pl.loop(NCH - ahead, NCH)
    def _(j):
        arrive(j)

    @pl.when(owner)
    def _():
        drain(gr.at[pl.ds(0, NPLANE - 1), pl.ds(0, PER)], small_r.at[2])
        za[z, 0:PER, :] = jnp.sum(gr[:, 0:PER, :], 0)

        def z_share(k):
            mine = za.at[z, pl.ds(0, PER)]
            remote(mine, mine, small_s.at[4], small_r.at[4], z_device(z + k)).start()

        @pl.when(z != 0)
        def _():
            z_share(NZ - z)

        def z_other(k):
            @pl.when(rem(z + k, NZ) != 0)
            def _():
                z_share(k)

        z_other(NZ // 2)
        for k in range(1, NZ // 2):
            z_other(NZ // 2 - k)
            z_other(NZ // 2 + k)

    average = jnp.sum(mean[...], -1, keepdims=True) * (1.0 / DIM)

    @pl.loop(0, NCH)
    def _(j):
        cols = pl.ds(pl.multiple_of(j * WIDE, WIDE), WIDE)
        value = (gain_of(j) * own[j] - xhat_of(j) * average) * inv[:, 0:1]
        out_o[:, cols] = value.astype(BF16)

    drain(tz.at[pl.ds(0, NZL // GROUP - 1), pl.ds(0, 5)], small_r.at[6])
    tf[line, 0:5, :] = jnp.sum(tz[:, 0:5, :], 0)

    @pl.loop(1, NLINE)
    def _(k):
        line_copy(k, tf.at[line, pl.ds(0, 5)], tf.at[line, pl.ds(0, 5)], 3).start()

    drain(tf.at[pl.ds(0, NLINE - 1), pl.ds(0, 5)], small_r.at[3])
    for p in range(NLINE):
        taps_o[:, p * 128 : (p + 1) * 128] = tf[p, 0:4, :]
        bias_o[:, p * 128 : (p + 1) * 128] = tf[p, 4:5, :]

    @pl.when(has_next)
    def _():
        to_next.wait_send()

    @pl.when(has_prev)
    def _():
        for copy in to_prev:
            copy.wait_send()

    drain(ybuf.at[:, pl.ds(0, NY - 1)], ys_sem)
    drain(zs, zs_sem)
    drain(tr.at[pl.ds(0, NLINE - 1), pl.ds(0, 5)], small_s.at[0])
    drain(tn.at[pl.ds(0, GROUP - 1), pl.ds(0, 5)], small_s.at[1])
    drain(tz.at[pl.ds(0, NZL // GROUP - 1), pl.ds(0, 5)], small_s.at[6])
    drain(tf.at[pl.ds(0, NLINE - 1), pl.ds(0, 5)], small_s.at[3])

    @pl.when(owner)
    def _():
        drain(gr.at[pl.ds(0, NCH - 1), pl.ds(0, PER)], small_s.at[2])
        drain(za.at[pl.ds(0, NZ - 1), pl.ds(0, PER)], small_s.at[4])

    @pl.when(jnp.logical_not(owner))
    def _():
        drain(gr.at[pl.ds(0, NCH), pl.ds(0, PER)], small_s.at[2])

    @pl.when(owner)
    def _():
        drain(za.at[pl.ds(0, NZ - 1), pl.ds(0, PER)], small_r.at[4])
        ga[place, 0:PER, :] = jnp.sum(za[:, 0:PER, :], 0)

        mine = ga.at[place, pl.ds(0, PER)]
        for i, j in reversed(CHIPS):
            for core in reversed(range(NC)):
                here = (x == i) & (y == j) & (c == core)

                @pl.when(jnp.logical_not(here))
                def _():
                    to = {"x": i, "y": j, "c": core}
                    remote(mine, mine, small_s.at[5], small_r.at[5], to).start()

    @pl.when(owner)
    def _():
        drain(ga.at[pl.ds(0, NCH - 1), pl.ds(0, PER)], small_r.at[5])

    @pl.when(jnp.logical_not(owner))
    def _():
        drain(ga.at[pl.ds(0, NCH), pl.ds(0, PER)], small_r.at[5])

    gain_o[...] = ga[:, 0:PER, :]

    @pl.when(owner)
    def _():
        drain(gr.at[pl.ds(0, NPLANE - 1), pl.ds(0, PER)], small_s.at[5])


def hand_on(*arrays):
    count = len(arrays)

    def body(*refs):
        sem = refs[2 * count]
        copies = [pltpu.make_async_copy(refs[i], refs[count + i], sem.at[i]) for i in range(count)]
        for copy in copies:
            copy.start()
        for copy in copies:
            copy.wait()

    return pl.pallas_call(
        body,
        out_shape=tuple(jax.ShapeDtypeStruct(a.shape, a.dtype) for a in arrays),
        in_specs=[pl.BlockSpec(memory_space=pltpu.VMEM)] * count,
        out_specs=(pl.BlockSpec(memory_space=pltpu.HBM),) * count,
        scratch_shapes=[pltpu.SemaphoreType.DMA((count,))],
        compiler_params=pltpu.CompilerParams(vmem_limit_bytes=4 << 20),
        name="hand_on",
    )(*arrays)


def on_device(hidden_in, norm_gain, proj_weight, conv_in, conv_weight, conv_bias, act_grad):
    vmem = pltpu.VMEM
    dma = pltpu.SemaphoreType.DMA
    out, gain, taps, bias = pl.pallas_call(
        kernel,
        out_shape=(
            jax.ShapeDtypeStruct((OWN, DIM), BF16),
            jax.ShapeDtypeStruct((NCH, PER, 128), F32),
            jax.ShapeDtypeStruct((4, CHAN), F32),
            jax.ShapeDtypeStruct((1, CHAN), F32),
        ),
        in_specs=[pl.BlockSpec(memory_space=pltpu.HBM)] * 7,
        out_specs=(pl.BlockSpec(memory_space=vmem),) * 4,
        scratch_shapes=[
            vmem((OWN, DIM), BF16),
            vmem((1, DIM), F32),
            vmem((DIM, CHAN), BF16),
            vmem((ROWS, CHAN), BF16),
            vmem((4, CHAN), F32),
            vmem((1, CHAN), F32),
            vmem((ROWS, CHAN), BF16),
            vmem((16, CHAN), BF16),
            vmem((16, CHAN), BF16),
            vmem((16, CHAN), BF16),
            vmem((ROWS + 16, CHAN), F32),
            vmem((ROWS + 8, CHAN), F32),
            vmem((ROWS, CHAN), BF16),
            vmem((5, 8, CHAN), F32),
            vmem((NCH, ROWS, WIDE), BF16),
            vmem((NCH, NY, PAIR, WIDE), BF16),
            vmem((NCH, OWN, WIDE), F32),
            vmem((NCH, OWN, WIDE), BF16),
            vmem((NCH, OWN, WIDE), BF16),
            vmem((OWN, 128), F32),
            vmem((OWN, 128), F32),
            vmem((NCH, 8, 128), F32),
            vmem((NPLANE, 8, 128), F32),
            vmem((NZ, 8, 128), F32),
            vmem((NCH, 8, 128), F32),
            vmem((NLINE, 8, 128), F32),
            vmem((NLINE, 8, 128), F32),
            vmem((GROUP, 8, 128), F32),
            vmem((NZL // GROUP, 8, 128), F32),
            vmem((NLINE, 8, 128), F32),
            dma((6,)),
            dma((WLOADS,)),
            dma((3,)),
            dma((3,)),
            dma,
            dma((NCH,)),
            dma,
            dma((NCH,)),
            dma((7,)),
            dma((7,)),
            pltpu.SemaphoreType.REGULAR((4,)),
        ],
        compiler_params=pltpu.CompilerParams(collective_id=0, has_side_effects=True, vmem_limit_bytes=40 << 20),
        name="layer_backward",
    )(
        *(
            pltpu.with_memory_space_constraint(a, pltpu.HBM)
            for a in (
                hidden_in,
                norm_gain.reshape(1, DIM),
                proj_weight,
                conv_in,
                conv_weight,
                conv_bias.reshape(1, CHAN),
                act_grad,
            )
        )
    )
    out, gain, taps, bias = hand_on(out, gain, taps, bias)
    return out, gain.reshape(DIM), taps, bias.reshape(CHAN)


def solution(mesh):
    finer = Mesh(mesh.devices.reshape(NZL, NX, NC, NY, NZH), ("zl", "x", "c", "y", "zh"))
    ctx = ("zl", "x", "c")
    tp = ("y", "zh")
    return jax.shard_map(
        on_device,
        mesh=finer,
        in_specs=(
            P(ctx + tp, None),
            P(),
            P(None, tp),
            P(ctx, tp),
            P(None, tp),
            P(tp),
            P(ctx, tp),
        ),
        out_specs=(P(ctx + tp, None), P(), P(None, tp), P(tp)),
        check_vma=False,
    )
```
